128 devices in a mesh: win: 8 (over z, core), step: 16 (over x, y).
Axes of the slice: x: 4, y: 4, z: 4, core: 2. Of those that a mesh axis runs over, the one named last changes fastest.
Arguments:
- initial_state: float32 [32, 32, 128], replicated, may hold values from -6 to 6
- source: float32 [8, 16, 32, 32, 128], P('win', 'step'), may hold values from -6 to 6
- absorption: float32 [32, 32, 128], replicated, may hold values from 0.01 to 0.2
Outputs:
- state: float32 [8, 16, 32, 32, 128], P('win', 'step')
The draws below stay inside these ranges and needn't reach their ends.
All inputs are finite; a program needn't handle non-finite values.
Results may differ from the reference program's by a relative error of at most 0.00026.
Values sent between devices are 32-bit elements; how exact they have to be, the bound alone decides.
A program may use at most 64 MiB of HBM per device.

```python
import math
import jax
import jax.numpy as jnp

NX = 32
NY = 32
NZ = 128
ITERS = 2
SWEEPS = 8
STEPS = 16
WINDOWS = 8


def block_scale(rng, dims, split, low, largest):
    def one(dim, blocks):
        heights = jax.random.uniform(jax.random.fold_in(jax.random.fold_in(rng, 6), dim), (blocks,), jnp.float32, low / len(split), largest / len(split))
        return jnp.repeat(jnp.exp(heights), dims[dim] // blocks).reshape((-1,) + (1,) * (len(dims) - dim - 1))

    loudness = one(*split[0])
    for cut in split[1:]:
        loudness = loudness * one(*cut)
    return loudness


def centred(own_key, extent, spread, most, shards=(), kind=jnp.bfloat16):
    factor_of = block_scale(own_key, extent, shards, -0.22, 0.18) if shards else 1.0
    values = jax.random.normal(own_key, extent, jnp.float32) * spread * factor_of
    return jnp.minimum(jnp.maximum(values, -most), most).astype(kind)


def setup_inputs(seed: int = 0) -> dict:
    keys = jax.random.split(jax.random.key(seed), 4)
    initial_state = centred(keys[0], (NX, NY, NZ), 1.0, 6.0, (), jnp.float32)
    source = centred(keys[1], (WINDOWS, STEPS, NX, NY, NZ), 1.0, 6.0, ((0, 8), (1, 16)), jnp.float32)
    absorption = jnp.clip(jnp.exp(jax.random.uniform(keys[2], (NX, NY, NZ), jnp.float32, math.log(0.01), math.log(0.2))), 0.01, 0.2)
    return dict(initial_state=initial_state, source=source, absorption=absorption)


alpha_corner = 0.1
coupling = 0.05


def pad_cube(field):
    widths = [(0, 0)] * (field.ndim - 3) + [(1, 1)] * 3
    return jnp.pad(field, widths)


def neighbours(field):
    padded = pad_cube(field)
    total = padded[..., 2:, 1:-1, 1:-1] + padded[..., :-2, 1:-1, 1:-1]
    total = total + padded[..., 1:-1, 2:, 1:-1] + padded[..., 1:-1, :-2, 1:-1]
    total = total + padded[..., 1:-1, 1:-1, 2:] + padded[..., 1:-1, 1:-1, :-2]
    return total


def complex_times(first, second):
    return jnp.stack([first[0] * second[0] - first[1] * second[1], first[0] * second[1] + first[1] * second[0]])


def relax(spectrum, inverse):
    field = complex_times(inverse, spectrum)
    for repeat in range(SWEEPS - 1):
        field = complex_times(inverse, spectrum + coupling * neighbours(field))
    return field


def inverse_diagonal(angle, absorption, gamma):
    real_part = 1.0 - gamma * jnp.cos(angle) + absorption + 6.0 * coupling
    imag_part = jnp.broadcast_to(gamma * jnp.sin(angle), real_part.shape)
    magnitude = real_part * real_part + imag_part * imag_part
    return jnp.stack([real_part / magnitude, -imag_part / magnitude])


def reference(initial_state, source, absorption):
    gamma = alpha_corner ** (1.0 / STEPS)
    moments = jnp.arange(STEPS, dtype=jnp.float32)
    scale = (gamma ** moments)[None, :, None, None, None]
    angle = (moments * (2.0 * math.pi / STEPS))[:, None, None, None]
    inverse = inverse_diagonal(angle, absorption, gamma)[:, None]
    state = jnp.zeros_like(source)
    for repeat in range(ITERS):
        ends = state[:, -1]
        before = jnp.concatenate([initial_state[None], ends[:-1]], axis=0)
        forcing = source.at[:, 0].add(before - alpha_corner * ends)
        spectrum_full = jnp.fft.fft(forcing * scale, axis=1)
        field = relax(jnp.stack([spectrum_full.real, spectrum_full.imag]), inverse)
        state = jnp.fft.ifft(field[0] + 1j * field[1], axis=1).real / scale
    return state
```

```python
import functools
import math

import jax
import jax.numpy as jnp
from jax import lax
from jax.experimental import pallas as pl
from jax.experimental.pallas import tpu as pltpu
from jax.sharding import PartitionSpec as P

SWEEPS = 8
STEPS = 16
WINDOWS = 8
SLOTS = 8
ALPHA = 0.1
COUPLING = 0.05
GAMMA = ALPHA ** (1.0 / STEPS)
NX, NY, NZ = 32, 32, 128
B = 8
MESH = pl.DeviceIdType.MESH
F32 = jnp.float32


def wpow(n, k):
    angle = 2.0 * math.pi * k / n
    return math.cos(angle), -math.sin(angle)


def times(c, s, re, im):
    if abs(s) < 1e-12:
        return (re, im) if c > 0 else (-re, None if im is None else -im)
    if abs(c) < 1e-12:
        if im is None:
            return None, (re if s > 0 else -re)
        return (-im, re) if s > 0 else (im, -re)
    if im is None:
        return c * re, s * re
    if abs(abs(c) - abs(s)) < 1e-12:
        h = abs(c)
        a, b = (re if c > 0 else -re), (im if c > 0 else -im)
        if c * s > 0:
            return h * (a - b), h * (b + a)
        return h * (a + b), h * (b - a)
    return c * re - s * im, c * im + s * re


def plus(a, b):
    return b if a is None else a if b is None else a + b


def minus(a, b):
    if b is None:
        return a
    return -b if a is None else a - b


def rdft(values):
    n = len(values)
    if n == 1:
        return [(values[0], None)]
    half = n // 2
    even, odd = rdft(values[0::2]), rdft(values[1::2])
    out = []
    for k in range(half + 1):
        if k == half:
            out.append((even[0][0] - odd[0][0], None))
            break
        if k <= half // 2:
            e, o = even[k], odd[k]
        else:
            e, o = even[half - k], odd[half - k]
            e = (e[0], None if e[1] is None else -e[1])
            o = (o[0], None if o[1] is None else -o[1])
        o = times(*wpow(n, k), *o)
        out.append((plus(e[0], o[0]), plus(e[1], o[1])))
    return out


def irdft(spectrum, n):
    if n == 1:
        return [spectrum[0][0]]
    half = n // 2
    even, odd = [], []
    for k in range(half // 2 + 1):
        x = spectrum[k]
        y = spectrum[half - k]
        ym = None if y[1] is None else -y[1]
        e = (plus(x[0], y[0]), plus(x[1], ym))
        d = (minus(x[0], y[0]), minus(x[1], ym))
        c, s = wpow(n, k)
        if 2 * k == half and half > 1:
            e = (x[0] + x[0], None)
            d = (None, x[1] + x[1])
        o = d if k == 0 else times_any(c, -s, *d)
        if k == 0 or 2 * k == half:
            e, o = (e[0], None), (o[0], None)
        even.append(e)
        odd.append(o)
    if half == 1:
        even, odd = even[:1], odd[:1]
    a, b = irdft(even, half), irdft(odd, half)
    out = [None] * n
    out[0::2], out[1::2] = a, b
    return out


def times_any(c, s, re, im):
    if re is None:
        r, i = times(c, s, im, None)
        return (None if i is None else -i), r
    return times(c, s, re, im)


def table(values, index):
    out = jnp.float32(values[0])
    for k in range(1, len(values)):
        out = jnp.where(index == k, jnp.float32(values[k]), out)
    return out


def kernel(
    src_hbm, init_hbm, abs_hbm, out_ref,
    src, ab, init, tbuf, sbuf, spec, kc, uu, ee, epart, ends, before, dext, kx, vv, f1, obuf,
    lsem, t1s, t1r, t2s, t2r, rss, rsr, wns, wnr, has, har, t3s, t3r, t4s, t4r,
):
    s = lax.axis_index("step")
    w = lax.axis_index("win")
    bx, by = s // 4, s % 4
    core = w % 2
    x0 = pl.multiple_of(bx * B, B)
    y0 = pl.multiple_of(by * B, B)
    slot = s // 2
    active = (bx + by + core) % 2 == 0

    def slot_device(f):
        return 2 * f + (f // 2 + core) % 2

    def origin(d):
        return pl.multiple_of((d // 4) * B, B), pl.multiple_of((d % 4) * B, B)

    def remote(source, target, send, recv, step=None, win=None):
        return pltpu.make_async_remote_copy(
            source, target, send, recv,
            device_id={"step": s if step is None else step, "win": w if win is None else win},
            device_id_type=MESH,
        )

    load_src = pltpu.make_async_copy(src_hbm, src, lsem.at[0])
    load_abs = pltpu.make_async_copy(abs_hbm, ab, lsem.at[1])
    load_init = pltpu.make_async_copy(init_hbm.at[pl.ds(x0, B), pl.ds(y0, B)], init, lsem.at[2])
    load_src.start()
    load_abs.start()
    load_init.start()

    barrier = pltpu.get_barrier_semaphore()
    for k in range(1, STEPS):
        pl.semaphore_signal(barrier, inc=1, device_id={"step": (s + k) % STEPS, "win": w}, device_id_type=MESH)
    for k in (1, WINDOWS - 1):
        pl.semaphore_signal(barrier, inc=1, device_id={"step": s, "win": (w + k) % WINDOWS}, device_id_type=MESH)
    pl.semaphore_wait(barrier, STEPS - 1 + 2)
    load_src.wait()

    t1 = []
    for k in range(1, STEPS):
        d = (s + k) % STEPS
        dx, dy = origin(d)
        copy = remote(src.at[pl.ds(dx, B), pl.ds(dy, B)], tbuf.at[s], t1s.at[k], t1r.at[s], step=d)
        copy.start()
        t1.append(copy)
    load_init.wait()
    load_abs.wait()
    tbuf[s] = src[pl.ds(x0, B), pl.ds(y0, B), :]

    cos_of = [math.cos(2 * math.pi * f / STEPS) for f in range(SLOTS)]
    sin_of = [math.sin(2 * math.pi * f / STEPS) for f in range(SLOTS)]
    c1 = table(cos_of, slot)
    c2 = table([-1.0] + cos_of[1:], slot)
    sn = table([0.0] + sin_of[1:], slot)

    def coefficients(a, cos1, cos2, sin):
        base = a + (1.0 + 6.0 * COUPLING)
        r1 = base - GAMMA * cos1
        im = GAMMA * sin
        scale1 = COUPLING / (r1 * r1 + im * im)
        r2 = base - GAMMA * cos2
        scale2 = COUPLING / (r2 * r2 + im * im)
        return r1 * scale1, r2 * scale2, -im * scale1

    @pl.when(active)
    def _():
        def plane(x, c):
            k1, k2, kb = coefficients(ab[x], c1, c2, sn)
            kc[0, x], kc[1, x], kc[2, x] = k1, k2, kb
            return c

        lax.fori_loop(0, NX, plane, 0, unroll=4)
        zero = jnp.zeros((48, NZ), F32)
        zrow = jnp.zeros((8, NZ), F32)
        for p in range(2):
            for c in range(2):
                uu[p, c, 0] = zero
                uu[p, c, NX + 1] = zero

        def rows(x, c):
            for p in range(2):
                for q in range(2):
                    uu[p, q, x, pl.ds(0, 8), :] = zrow
                    uu[p, q, x, pl.ds(40, 8), :] = zrow
            return c

        lax.fori_loop(1, NX + 1, rows, 0, unroll=4)

    def wide_plane(i, c):
        gx = x0 - B + i
        inx = jnp.logical_and(gx >= 0, gx < NX)
        gxc = jnp.clip(gx, 0, NX - 1)
        for b in range(3):
            gy = by - 1 + b
            inside = jnp.logical_and(inx, jnp.logical_and(gy >= 0, gy < 4))
            keep = jnp.where(inside, jnp.float32(1.0), jnp.float32(0.0))
            a = ab[gxc, pl.ds(pl.multiple_of(jnp.clip(gy, 0, 3) * B, B), B), :]
            for f in range(SLOTS):
                if f == 0:
                    first = keep * COUPLING / (a + (1.0 + 6.0 * COUPLING - GAMMA))
                    second = keep * COUPLING / (a + (1.0 + 6.0 * COUPLING + GAMMA))
                else:
                    r = a + (1.0 + 6.0 * COUPLING - GAMMA * cos_of[f])
                    im = GAMMA * sin_of[f]
                    scale = keep * COUPLING / (r * r + im * im)
                    first, second = r * scale, -im * scale
                kx[f, 0, i, pl.ds(b * B, B), :] = first
                kx[f, 1, i, pl.ds(b * B, B), :] = second
        return c

    lax.fori_loop(0, 3 * B, wide_plane, 0)

    for k in range(1, STEPS):
        d = (s - k) % STEPS
        remote(src.at[pl.ds(0, B), pl.ds(0, B)], tbuf.at[d], t1s.at[k], t1r.at[d], step=d).wait_recv()
    first_window = jnp.where(w == 0, jnp.float32(1.0), jnp.float32(0.0))

    def transform(x, c):
        values = []
        for t in range(STEPS):
            v = tbuf[t, x]
            if t == 0:
                v = v + first_window * init[x]
            values.append(v * (GAMMA**t / COUPLING))
        out = rdft(values)
        sbuf[0, 0, x], sbuf[0, 1, x] = out[0][0], out[8][0]
        for f in range(1, SLOTS):
            sbuf[f, 0, x], sbuf[f, 1, x] = out[f]
        return c

    lax.fori_loop(0, B, transform, 0)

    t2 = []
    for k in range(1, SLOTS):
        f = (slot + k) % SLOTS
        copy = remote(
            sbuf.at[f], spec.at[:, pl.ds(x0, B), pl.ds(y0, B)], t2s.at[k], t2r.at[s], step=slot_device(f)
        )
        copy.start()
        t2.append(copy)
    partner = s + 1 - 2 * (s % 2)
    to_partner = remote(
        sbuf.at[slot], spec.at[:, pl.ds(x0, B), pl.ds(y0, B)], t2s.at[0], t2r.at[s], step=partner
    )

    @pl.when(jnp.logical_not(active))
    def _():
        to_partner.start()

    @pl.when(active)
    def _():
        for c in range(2):
            spec[c, pl.ds(x0, B), pl.ds(y0, B), :] = sbuf[slot, c]
        for k in range(1, STEPS):
            d = (s + k) % STEPS
            dx, dy = origin(d)
            remote(
                sbuf.at[slot], spec.at[:, pl.ds(dx, B), pl.ds(dy, B)], t2s.at[0], t2r.at[d], step=d
            ).wait_recv()

    lane = lax.broadcasted_iota(jnp.int32, (8, NZ), 1)

    def z_sum(v):
        n = v.shape[0]
        at = jnp.concatenate([lane] * (n // 8), 0) if n > 8 else lane
        below = jnp.where(at == 0, 0.0, pltpu.roll(v, 1, 1))
        above = jnp.where(at == NZ - 1, 0.0, pltpu.roll(v, NZ - 1, 1))
        return below + above

    def neighbours(load, x, y, n):
        total = load(x - 1, y, n) + load(x + 1, y, n)
        total = total + (load(x, y - 1, n) + load(x, y + 1, n))
        return total + z_sum(load(x, y, n))

    p_end = 2.0 / (16 * GAMMA**15)
    ends_re = table([0.5 * p_end] + [p_end * v for v in cos_of[1:]], slot)
    ends_im = table([-0.5 * p_end] + [p_end * v for v in sin_of[1:]], slot)

    @pl.when(active)
    def _():
        def start(x, c):
            k1, k2, kb = kc[0, x], kc[1, x], kc[2, x]
            s0, s1 = spec[0, x], spec[1, x]
            uu[0, 0, x + 1, pl.ds(8, NY), :] = k1 * s0 - kb * s1
            uu[0, 1, x + 1, pl.ds(8, NY), :] = k2 * s1 + kb * s0
            return c

        lax.fori_loop(0, NX, start, 0, unroll=4)

        def sweep(k, c):
            old = k % 2
            for x in range(NX):
                nb = [
                    neighbours(
                        lambda px, py, n, q=q: uu[old, q, px, pl.ds(py, n), :], x + 1, 8, NY
                    )
                    for q in range(2)
                ]
                k1, k2, kb = kc[0, x], kc[1, x], kc[2, x]
                s0, s1 = spec[0, x] + nb[0], spec[1, x] + nb[1]
                uu[1 - old, 0, x + 1, pl.ds(8, NY), :] = k1 * s0 - kb * s1
                uu[1 - old, 1, x + 1, pl.ds(8, NY), :] = k2 * s1 + kb * s0
            return c

        lax.fori_loop(0, SWEEPS - 1, sweep, 0)

        def end(x, c):
            rows = pl.ds(8, NY)
            ee[x] = ends_re * uu[1, 0, x + 1, rows, :] + ends_im * uu[1, 1, x + 1, rows, :]
            return c

        lax.fori_loop(0, NX, end, 0, unroll=4)

        for k in range(1, STEPS):
            d = (s + k) % STEPS
            dx, dy = origin(d)
            remote(ee.at[pl.ds(dx, B), pl.ds(dy, B)], epart.at[slot], rss.at[k], rsr.at[slot], step=d).start()
        epart[slot] = ee[pl.ds(x0, B), pl.ds(y0, B), :]

    def slots_wait(wait):
        for k in range(1, SLOTS):
            f = (slot + k) % SLOTS
            wait(f, slot_device(f))
        pl.when(jnp.logical_not(active))(lambda: wait(slot, partner))

    block = (pl.ds(0, B), pl.ds(0, B))
    slots_wait(lambda f, d: remote(ee.at[block], epart.at[f], rss.at[0], rsr.at[f], step=d).wait_recv())
    for x in range(B):
        total = epart[0, x]
        for f in range(1, SLOTS):
            total = total + epart[f, x]
        ends[x] = total

    to_next = remote(ends, before, wns.at[0], wnr.at[0], win=(w + 1) % WINDOWS)
    to_next.start()
    to_next.wait_recv()
    later_window = jnp.where(w == 0, jnp.float32(0.0), jnp.float32(1.0 / COUPLING))
    for x in range(B):
        dext[B + x, pl.ds(B, B), :] = later_window * before[x] - (ALPHA / COUPLING) * ends[x]

    shifts = [(i, j) for i in (-1, 0, 1) for j in (-1, 0, 1) if (i, j) != (0, 0)]
    centre = dext.at[pl.ds(B, B), pl.ds(B, B)]
    halo = []
    for k, (i, j) in enumerate(shifts):
        d = ((bx + i + 4) % 4) * 4 + (by + j + 4) % 4
        copy = remote(
            centre, dext.at[pl.ds(B - B * i, B), pl.ds(B - B * j, B)], has.at[k], har.at[k], step=d
        )
        copy.start()
        halo.append(copy)

    @pl.when(active)
    def _():
        for k in range(1, STEPS):
            d = (s + k) % STEPS
            dx, dy = origin(d)
            remote(
                uu.at[1, :, pl.ds(dx + 1, B), pl.ds(pl.multiple_of(dy + 8, 8), B)],
                f1.at[slot], t3s.at[k], t3r.at[slot], step=d,
            ).start()
        for c in range(2):
            f1[slot, c] = uu[1, c, pl.ds(x0 + 1, B), pl.ds(pl.multiple_of(y0 + 8, 8), B), :]

    for copy in halo:
        copy.wait_recv()

    def wide_start(i, c):
        rows = pl.ds(0, 3 * B)
        d = dext[i, rows, :]
        for f in range(SLOTS):
            vv[0, f, 0, i, rows, :] = kx[f, 0, i, rows, :] * d
            vv[0, f, 1, i, rows, :] = kx[f, 1, i, rows, :] * d
        return c

    lax.fori_loop(0, 3 * B, wide_start, 0)
    for k in range(SWEEPS - 1):
        reach = SWEEPS - 2 - k
        old, new = k % 2, 1 - k % 2
        n = -(-(B + 2 * reach) // 8) * 8
        y = B - reach

        def wide(i, c, old=old, new=new, n=n, y=y):
            rows = pl.ds(y, n)
            d = dext[i, rows, :]
            for f in range(SLOTS):
                nb = [
                    neighbours(lambda px, py, m, q=q: vv[old, f, q, px, pl.ds(py, m), :], i, y, n)
                    for q in range(2)
                ]
                ka, kb = kx[f, 0, i, rows, :], kx[f, 1, i, rows, :]
                s0 = d + nb[0]
                if f == 0:
                    re, im = ka * s0, kb * (d + nb[1])
                else:
                    re, im = ka * s0 - kb * nb[1], ka * nb[1] + kb * s0
                vv[new, f, 0, i, rows, :] = re
                vv[new, f, 1, i, rows, :] = im
            return c

        lax.fori_loop(B - reach, 2 * B + reach, wide, 0, unroll=2)

    slots_wait(
        lambda f, d: remote(uu.at[1, :, pl.ds(0, B), pl.ds(0, B)], f1.at[f], t3s.at[0], t3r.at[f], step=d).wait_recv()
    )

    def untransform(x, c):
        total = [
            [f1[f, q, x] + vv[1, f, q, B + x, pl.ds(B, B), :] for q in range(2)] for f in range(SLOTS)
        ]
        spectrum = [(total[0][0], None)] + [tuple(v) for v in total[1:]] + [(total[0][1], None)]
        values = irdft(spectrum, STEPS)
        for t in range(STEPS):
            obuf[t, x] = values[t] * (GAMMA ** (-t) / STEPS)
        return c

    lax.fori_loop(0, B, untransform, 0)
    t4 = []
    for k in range(1, STEPS):
        d = (s + k) % STEPS
        copy = remote(obuf.at[d], out_ref.at[pl.ds(x0, B), pl.ds(y0, B)], t4s.at[k], t4r.at[s], step=d)
        copy.start()
        t4.append(copy)
    out_ref[pl.ds(x0, B), pl.ds(y0, B), :] = obuf[s]

    for copy in t1 + t2:
        copy.wait_send()
    pl.when(jnp.logical_not(active))(to_partner.wait_send)
    to_next.wait_send()
    for copy in halo:
        copy.wait_send()

    @pl.when(active)
    def _():
        for k in range(1, STEPS):
            d = (s + k) % STEPS
            remote(ee.at[block], epart.at[slot], rss.at[k], rsr.at[slot], step=d).wait_send()
            remote(
                uu.at[1, :, pl.ds(0, B), pl.ds(0, B)], f1.at[slot], t3s.at[k], t3r.at[slot], step=d
            ).wait_send()

    for k in range(1, STEPS):
        d = (s + k) % STEPS
        dx, dy = origin(d)
        remote(obuf.at[d], out_ref.at[pl.ds(dx, B), pl.ds(dy, B)], t4s.at[k], t4r.at[d], step=d).wait_recv()
    for copy in t4:
        copy.wait_send()


def per_device(initial_state, source, absorption):
    grid = (NX, NY, NZ)
    vmem = lambda *shape: pltpu.VMEM(shape, F32)
    dma = lambda n: pltpu.SemaphoreType.DMA((n,))
    result = pl.pallas_call(
        kernel,
        out_shape=jax.ShapeDtypeStruct(grid, F32),
        in_specs=[pl.BlockSpec(memory_space=pl.ANY)] * 3,
        out_specs=pl.BlockSpec(memory_space=pltpu.VMEM),
        scratch_shapes=[
            vmem(*grid),
            vmem(*grid),
            vmem(B, B, NZ),
            vmem(STEPS, B, B, NZ),
            vmem(SLOTS, 2, B, B, NZ),
            vmem(2, *grid),
            vmem(3, *grid),
            vmem(2, 2, NX + 2, NY + 16, NZ),
            vmem(*grid),
            vmem(SLOTS, B, B, NZ),
            vmem(B, B, NZ),
            vmem(B, B, NZ),
            vmem(3 * B, 4 * B, NZ),
            vmem(SLOTS, 2, 3 * B, 4 * B, NZ),
            vmem(2, SLOTS, 2, 3 * B, 4 * B, NZ),
            vmem(SLOTS, 2, B, B, NZ),
            vmem(STEPS, B, B, NZ),
            dma(3),
            dma(STEPS), dma(STEPS),
            dma(SLOTS), dma(STEPS),
            dma(STEPS), dma(SLOTS),
            dma(1), dma(1),
            dma(8), dma(8),
            dma(STEPS), dma(SLOTS),
            dma(STEPS), dma(STEPS),
        ],
        compiler_params=pltpu.CompilerParams(
            collective_id=0, has_side_effects=True, vmem_limit_bytes=60 * 2**20
        ),
        name="windows",
    )(source[0, 0], initial_state, absorption)
    return result[None, None]


def solution(mesh):
    return jax.shard_map(
        per_device,
        mesh=mesh,
        in_specs=(P(), P("win", "step", None, None, None), P()),
        out_specs=P("win", "step", None, None, None),
        check_vma=False,
    )
```

```python
import functools
import math

import jax
import jax.numpy as jnp
from jax import lax
from jax.experimental import pallas as pl
from jax.experimental.pallas import tpu as pltpu
from jax.sharding import PartitionSpec as P

SWEEPS = 8
STEPS = 16
WINDOWS = 8
SLOTS = 8
PAIRS = 4
GROUPS = (5, 6, 8, 7, 6, 10, 8)
PITCH = 32
ALPHA = 0.1
COUPLING = 0.05
GAMMA = ALPHA ** (1.0 / STEPS)
NX, NY, NZ = 32, 32, 128
B = 8
MESH = pl.DeviceIdType.MESH
F32 = jnp.float32
BF16 = jnp.bfloat16
HALF = NZ // 2


def wpow(n, k):
    angle = 2.0 * math.pi * k / n
    return math.cos(angle), -math.sin(angle)


def times(c, s, re, im):
    if abs(s) < 1e-12:
        return (re, im) if c > 0 else (-re, None if im is None else -im)
    if abs(c) < 1e-12:
        if im is None:
            return None, (re if s > 0 else -re)
        return (-im, re) if s > 0 else (im, -re)
    if im is None:
        return c * re, s * re
    if abs(abs(c) - abs(s)) < 1e-12:
        h = abs(c)
        a, b = (re if c > 0 else -re), (im if c > 0 else -im)
        if c * s > 0:
            return h * (a - b), h * (b + a)
        return h * (a + b), h * (b - a)
    return c * re - s * im, c * im + s * re


def plus(a, b):
    return b if a is None else a if b is None else a + b


def minus(a, b):
    if b is None:
        return a
    return -b if a is None else a - b


def rdft(values):
    n = len(values)
    if n == 1:
        return [(values[0], None)]
    half = n // 2
    even, odd = rdft(values[0::2]), rdft(values[1::2])
    out = []
    for k in range(half + 1):
        if k == half:
            out.append((even[0][0] - odd[0][0], None))
            break
        if k <= half // 2:
            e, o = even[k], odd[k]
        else:
            e, o = even[half - k], odd[half - k]
            e = (e[0], None if e[1] is None else -e[1])
            o = (o[0], None if o[1] is None else -o[1])
        o = times(*wpow(n, k), *o)
        out.append((plus(e[0], o[0]), plus(e[1], o[1])))
    return out


def irdft(spectrum, n):
    if n == 1:
        return [spectrum[0][0]]
    half = n // 2
    even, odd = [], []
    for k in range(half // 2 + 1):
        x = spectrum[k]
        y = spectrum[half - k]
        ym = None if y[1] is None else -y[1]
        e = (plus(x[0], y[0]), plus(x[1], ym))
        d = (minus(x[0], y[0]), minus(x[1], ym))
        c, s = wpow(n, k)
        if 2 * k == half and half > 1:
            e = (x[0] + x[0], None)
            d = (None, x[1] + x[1])
        o = d if k == 0 else times_any(c, -s, *d)
        if k == 0 or 2 * k == half:
            e, o = (e[0], None), (o[0], None)
        even.append(e)
        odd.append(o)
    if half == 1:
        even, odd = even[:1], odd[:1]
    a, b = irdft(even, half), irdft(odd, half)
    out = [None] * n
    out[0::2], out[1::2] = a, b
    return out


def times_any(c, s, re, im):
    if re is None:
        r, i = times(c, s, im, None)
        return (None if i is None else -i), r
    return times(c, s, re, im)


def part(p, odd, q):
    return p * 4 + odd * 2 + q


def kz(odd):
    return 16 + odd


def dd(which):
    return 18 + which


def spread(v, pick, terms=3):
    total = None
    for k in range(terms):
        part = v.astype(BF16)
        product = jnp.dot(part, pick, preferred_element_type=F32)
        total = product if total is None else total + product
        if k < terms - 1:
            v = v - part.astype(F32)
    return total


def table(values, index):
    out = jnp.float32(values[0])
    for k in range(1, len(values)):
        out = jnp.where(index == k, jnp.float32(values[k]), out)
    return out


def kernel(
    src_hbm, init_hbm, abs_hbm, out_ref,
    src, ab, init, tbuf, sbuf, spec, kc, uu, ee, epart, ends, before, dext, va, vb, kk, join, f1, obuf,
    lsem, t1s, t1r, t2s, t2r, rss, rsr, wns, wnr, has, har, t3s, t3r, t4s, t4r,
):
    s = lax.axis_index("step")
    w = lax.axis_index("win")
    bx, by = s // 4, s % 4
    core = w % 2
    x0 = pl.multiple_of(bx * B, B)
    y0 = pl.multiple_of(by * B, B)
    slot = s // 2
    active = (bx + by + core) % 2 == 0

    def slot_device(f):
        return 2 * f + (f // 2 + core) % 2

    def origin(d):
        return pl.multiple_of((d // 4) * B, B), pl.multiple_of((d % 4) * B, B)

    def remote(source, target, send, recv, step=None, win=None):
        return pltpu.make_async_remote_copy(
            source, target, send, recv,
            device_id={"step": s if step is None else step, "win": w if win is None else win},
            device_id_type=MESH,
        )

    load_src = pltpu.make_async_copy(src_hbm, src, lsem.at[0])
    load_abs = pltpu.make_async_copy(abs_hbm, ab, lsem.at[1])
    load_init = pltpu.make_async_copy(init_hbm.at[pl.ds(x0, B), pl.ds(y0, B)], init, lsem.at[2])
    load_src.start()
    load_abs.start()
    load_init.start()

    barrier = pltpu.get_barrier_semaphore()
    for k in range(1, STEPS):
        pl.semaphore_signal(barrier, inc=1, device_id={"step": (s + k) % STEPS, "win": w}, device_id_type=MESH)
    for k in (1, WINDOWS - 1):
        pl.semaphore_signal(barrier, inc=1, device_id={"step": s, "win": (w + k) % WINDOWS}, device_id_type=MESH)
    pl.semaphore_wait(barrier, STEPS - 1 + 2)
    load_src.wait()

    t1 = []
    for k in range(1, STEPS):
        d = (s + k) % STEPS
        dx, dy = origin(d)
        copy = remote(src.at[pl.ds(dx, B), pl.ds(dy, B)], tbuf.at[s], t1s.at[k], t1r.at[s], step=d)
        copy.start()
        t1.append(copy)
    load_init.wait()
    load_abs.wait()
    tbuf[s] = src[pl.ds(x0, B), pl.ds(y0, B), :]

    cos_of = [math.cos(2 * math.pi * f / STEPS) for f in range(SLOTS)]
    sin_of = [math.sin(2 * math.pi * f / STEPS) for f in range(SLOTS)]
    c1 = table(cos_of, slot)
    c2 = table([-1.0] + cos_of[1:], slot)
    sn = table([0.0] + sin_of[1:], slot)

    def coefficients(a, cos1, cos2, sin):
        base = a + (1.0 + 6.0 * COUPLING)
        r1 = base - GAMMA * cos1
        im = GAMMA * sin
        scale1 = COUPLING / (r1 * r1 + im * im)
        r2 = base - GAMMA * cos2
        scale2 = COUPLING / (r2 * r2 + im * im)
        return r1 * scale1, r2 * scale2, -im * scale1

    @pl.when(active)
    def _():
        def plane(x, c):
            k1, k2, kb = coefficients(ab[x], c1, c2, sn)
            for n, value in enumerate((k1, k2, kb)):
                kc[n, x, pl.ds(0, NY), :] = value
            return c

        lax.fori_loop(0, NX, plane, 0, unroll=4)
        zero = jnp.zeros((NY + 24, NZ), F32)
        zrow = jnp.zeros((8, NZ), F32)
        for p in range(2):
            for c in range(2):
                uu[p, c, 0] = zero
                uu[p, c, NX + 1] = zero

        def rows(x, c):
            for p in range(2):
                for q in range(2):
                    uu[p, q, x, pl.ds(0, 8), :] = zrow
                    uu[p, q, x, pl.ds(40, 8), :] = zrow
            return c

        lax.fori_loop(1, NX + 1, rows, 0, unroll=4)

    for k in range(1, STEPS):
        d = (s - k) % STEPS
        remote(src.at[pl.ds(0, B), pl.ds(0, B)], tbuf.at[d], t1s.at[k], t1r.at[d], step=d).wait_recv()
    first_window = jnp.where(w == 0, jnp.float32(1.0), jnp.float32(0.0))

    def transform(x, c):
        values = []
        for t in range(STEPS):
            v = tbuf[t, x]
            if t == 0:
                v = v + first_window * init[x]
            values.append(v * (GAMMA**t / COUPLING))
        out = rdft(values)
        sbuf[0, 0, x], sbuf[0, 1, x] = out[0][0], out[8][0]
        for f in range(1, SLOTS):
            sbuf[f, 0, x], sbuf[f, 1, x] = out[f]
        return c

    lax.fori_loop(0, B, transform, 0)

    t2 = []
    for k in range(1, SLOTS):
        f = (slot + k) % SLOTS
        copy = remote(
            sbuf.at[f], spec.at[:, pl.ds(x0, B), pl.ds(y0, B)], t2s.at[k], t2r.at[s], step=slot_device(f)
        )
        copy.start()
        t2.append(copy)
    partner = s + 1 - 2 * (s % 2)
    to_partner = remote(
        sbuf.at[slot], spec.at[:, pl.ds(x0, B), pl.ds(y0, B)], t2s.at[0], t2r.at[s], step=partner
    )

    @pl.when(jnp.logical_not(active))
    def _():
        to_partner.start()


    wide_lane = lax.broadcasted_iota(jnp.int32, (3 * B, NZ), 1)
    low = wide_lane < HALF
    pick_z = lax.broadcasted_iota(jnp.int32, (NZ, 2 * NZ), 0)
    pick_l = lax.broadcasted_iota(jnp.int32, (NZ, 2 * NZ), 1)
    pick = jnp.where(pick_z == 2 * (pick_l % HALF) + pick_l // NZ, 1.0, 0.0).astype(BF16)
    join_r = lax.broadcasted_iota(jnp.int32, (2 * NZ, 2 * NZ), 0)
    join_c = lax.broadcasted_iota(jnp.int32, (2 * NZ, 2 * NZ), 1)
    goes = ((join_r // HALF) % 2) * NZ + 2 * (join_r % HALF) + join_r // NZ
    join[...] = jnp.where(join_c == goes, 1.0, 0.0).astype(BF16)

    def at(a, b):
        return jnp.where(low, jnp.float32(a), jnp.float32(b))

    def turned(v, odd):
        lanes = wide_lane[: v.shape[0]] % HALF
        if odd:
            return jnp.where(lanes == 0, 0.0, pltpu.roll(v, 1, 1))
        return jnp.where(lanes == HALF - 1, 0.0, pltpu.roll(v, NZ - 1, 1))

    def wide_plane(i, c):
        gx = x0 - B + i
        inx = jnp.logical_and(gx >= 0, gx < NX)
        gxc = jnp.clip(gx, 0, NX - 1)
        tiles, keeps = [], []
        for b in range(3):
            gy = by - 1 + b
            inside = jnp.logical_and(inx, jnp.logical_and(gy >= 0, gy < 4))
            keep = jnp.where(inside, jnp.float32(COUPLING), jnp.float32(0.0))
            tiles.append(ab[gxc, pl.ds(pl.multiple_of(jnp.clip(gy, 0, 3) * B, B), B), :])
            keeps.append(jnp.full((B, NZ), keep, F32))
        both = spread(jnp.concatenate(tiles, 0), pick)
        keep = jnp.concatenate(keeps, 0)
        rows = pl.ds(pl.multiple_of(i * PITCH, PITCH), 3 * B)
        for odd in range(2):
            base = both[:, odd * NZ : (odd + 1) * NZ] + (1.0 + 6.0 * COUPLING)
            for p in range(PAIRS):
                q = p + PAIRS
                r = base - at(GAMMA * cos_of[p], GAMMA * cos_of[q])
                im = at(GAMMA * sin_of[p], GAMMA * sin_of[q])
                scale = keep / (r * r + im * im)
                ka, kb = r * scale, -im * scale
                if p == 0:
                    r2 = base - at(-GAMMA, GAMMA * cos_of[q])
                    k2 = r2 * (keep / (r2 * r2 + im * im))
                    kk[kz(odd), rows, :] = k2
                kk[part(p, odd, 0), rows, :], kk[part(p, odd, 1), rows, :] = ka, kb
        return c

    lax.fori_loop(1, 3 * B - 1, wide_plane, 0)

    @pl.when(active)
    def _():
        for c in range(2):
            spec[c, pl.ds(x0, B), pl.ds(y0, B), :] = sbuf[slot, c]
        for k in range(1, STEPS):
            d = (s + k) % STEPS
            dx, dy = origin(d)
            remote(
                sbuf.at[slot], spec.at[:, pl.ds(dx, B), pl.ds(dy, B)], t2s.at[0], t2r.at[d], step=d
            ).wait_recv()

    lane = lax.broadcasted_iota(jnp.int32, (8, NZ), 1)

    def z_sum(v):
        n = v.shape[0]
        at = jnp.concatenate([lane] * (n // 8), 0) if n > 8 else lane
        below = jnp.where(at == 0, 0.0, pltpu.roll(v, 1, 1))
        above = jnp.where(at == NZ - 1, 0.0, pltpu.roll(v, NZ - 1, 1))
        return below + above

    def neighbours(load, x, y, n):
        total = load(x - 1, y, n) + load(x + 1, y, n)
        total = total + (load(x, y - 1, n) + load(x, y + 1, n))
        return total + z_sum(load(x, y, n))

    p_end = 2.0 / (16 * GAMMA**15)
    ends_re = table([0.5 * p_end] + [p_end * v for v in cos_of[1:]], slot)
    ends_im = table([-0.5 * p_end] + [p_end * v for v in sin_of[1:]], slot)

    @pl.when(active)
    def _():
        def start(x, c):
            k1, k2, kb = (kc[n, x, pl.ds(0, NY), :] for n in range(3))
            s0, s1 = (spec[n, x, pl.ds(0, NY), :] for n in range(2))
            uu[0, 0, x + 1, pl.ds(8, NY), :] = k1 * s0 - kb * s1
            uu[0, 1, x + 1, pl.ds(8, NY), :] = k2 * s1 + kb * s0
            return c

        lax.fori_loop(0, NX, start, 0, unroll=4)

        def sweep(k, c):
            old = k % 2
            for x in range(NX):
                nb = [
                    neighbours(
                        lambda px, py, n, q=q: uu[old, q, px, pl.ds(py, n), :], x + 1, 8, NY
                    )
                    for q in range(2)
                ]
                k1, k2, kb = (kc[n, x, pl.ds(0, NY), :] for n in range(3))
                s0, s1 = (spec[n, x, pl.ds(0, NY), :] + nb[n] for n in range(2))
                uu[1 - old, 0, x + 1, pl.ds(8, NY), :] = k1 * s0 - kb * s1
                uu[1 - old, 1, x + 1, pl.ds(8, NY), :] = k2 * s1 + kb * s0
            return c

        lax.fori_loop(0, SWEEPS - 1, sweep, 0)

        def end(x, c):
            rows = pl.ds(8, NY)
            ee[x] = ends_re * uu[1, 0, x + 1, rows, :] + ends_im * uu[1, 1, x + 1, rows, :]
            return c

        lax.fori_loop(0, NX, end, 0, unroll=4)

        for k in range(1, STEPS):
            d = (s + k) % STEPS
            dx, dy = origin(d)
            remote(ee.at[pl.ds(dx, B), pl.ds(dy, B)], epart.at[slot], rss.at[k], rsr.at[slot], step=d).start()
        epart[slot] = ee[pl.ds(x0, B), pl.ds(y0, B), :]

    def slots_wait(wait):
        for k in range(1, SLOTS):
            f = (slot + k) % SLOTS
            wait(f, slot_device(f))
        pl.when(jnp.logical_not(active))(lambda: wait(slot, partner))

    block = (pl.ds(0, B), pl.ds(0, B))
    slots_wait(lambda f, d: remote(ee.at[block], epart.at[f], rss.at[0], rsr.at[f], step=d).wait_recv())
    for x in range(B):
        total = epart[0, x]
        for f in range(1, SLOTS):
            total = total + epart[f, x]
        ends[x] = total

    to_next = remote(ends, before, wns.at[0], wnr.at[0], win=(w + 1) % WINDOWS)
    to_next.start()
    @pl.when(active)
    def _():
        for k in range(1, STEPS):
            d = (s + k) % STEPS
            dx, dy = origin(d)
            remote(
                uu.at[1, :, pl.ds(dx + 1, B), pl.ds(pl.multiple_of(dy + 8, 8), B)],
                f1.at[slot], t3s.at[k], t3r.at[slot], step=d,
            ).start()
        for c in range(2):
            f1[slot, c] = uu[1, c, pl.ds(x0 + 1, B), pl.ds(pl.multiple_of(y0 + 8, 8), B), :]

    to_next.wait_recv()
    later_window = jnp.where(w == 0, jnp.float32(0.0), jnp.float32(1.0 / COUPLING))
    change = later_window * before[...] - (ALPHA / COUPLING) * ends[...]
    pack = jnp.where(
        pick_z[:, :NZ] == 2 * (pick_l[:, :NZ] % HALF) + pick_l[:, :NZ] // HALF, 1.0, 0.0
    ).astype(BF16)
    dext[pl.ds(B, B), pl.ds(B, B), :] = spread(change.reshape(B * B, NZ), pack).reshape(B, B, NZ)

    shifts = [(i, j) for i in (-1, 0, 1) for j in (-1, 0, 1) if (i, j) != (0, 0)]
    centre = dext.at[pl.ds(B, B), pl.ds(B, B)]
    halo = []
    for k, (i, j) in enumerate(shifts):
        d = ((bx + i + 4) % 4) * 4 + (by + j + 4) % 4
        copy = remote(
            centre, dext.at[pl.ds(B - B * i, B), pl.ds(B - B * j, B)], has.at[k], har.at[k], step=d
        )
        copy.start()
        halo.append(copy)

    for copy in halo:
        copy.wait_recv()

    def wide_start(i, c):
        rows = pl.ds(pl.multiple_of(i * PITCH, PITCH), 3 * B)
        v = dext[i, pl.ds(0, 3 * B), :]
        swapped = pltpu.roll(v, HALF, 1)
        d = [jnp.where(low, v, swapped), jnp.where(low, swapped, v)]
        for odd in range(2):
            kk[dd(odd), rows, :] = d[odd]
            kk[dd(2 + odd), rows, :] = jnp.where(low, d[odd], 0.0)
            for p in range(PAIRS):
                second = kk[part(p, odd, 1), rows, :]
                if p == 0:
                    second = jnp.where(low, kk[kz(odd), rows, :], second)
                va[part(p, odd, 0), rows, :] = kk[part(p, odd, 0), rows, :] * d[odd]
                va[part(p, odd, 1), rows, :] = second * d[odd]
        return c

    lax.fori_loop(1, 3 * B - 1, wide_start, 0)
    zero_row = s // STEPS
    for k in range(SWEEPS - 1):
        reach = SWEEPS - 2 - k
        vo, vn = (va, vb) if k % 2 == 0 else (vb, va)
        n = -(-(B + 2 * reach) // 8) * 8
        first_row = zero_row + (B - reach)
        group = GROUPS[k]

        def compute(start, n=n, vo=vo, vn=vn):
            rows = pl.ds(start, n)
            around = [pl.ds(start + shift, n) for shift in (-PITCH, PITCH, -1, 1)]
            for p in range(PAIRS):
                middle = [[vo[part(p, odd, q), rows, :] for q in range(2)] for odd in range(2)]
                for odd in range(2):
                    nb = []
                    for q in range(2):
                        here, other = part(p, odd, q), middle[1 - odd][q]
                        t = vo[here, around[0], :] + vo[here, around[1], :]
                        t = t + (vo[here, around[2], :] + vo[here, around[3], :])
                        nb.append((t + other) + turned(other, 1 - odd))
                    ka, kb = kk[part(p, odd, 0), rows, :], kk[part(p, odd, 1), rows, :]
                    s0, s1, k2 = kk[dd(odd), rows, :] + nb[0], nb[1], ka
                    if p == 0:
                        s1, k2 = s1 + kk[dd(2 + odd), rows, :], kk[kz(odd), rows, :]
                    vn[part(p, odd, 0), rows, :] = ka * s0 - kb * s1
                    vn[part(p, odd, 1), rows, :] = k2 * s1 + kb * s0

        def wide(j, c, reach=reach, compute=compute, group=group, first_row=first_row):
            start = (B - reach + group * j) * PITCH + first_row
            for m in range(group):
                for tile in range(n // 8):
                    compute(start + m * PITCH + tile * 8, 8)
            return c

        lax.fori_loop(0, (B + 2 * reach) // group, wide, 0)

    slots_wait(
        lambda f, d: remote(uu.at[1, :, pl.ds(0, B), pl.ds(0, B)], f1.at[f], t3s.at[0], t3r.at[f], step=d).wait_recv()
    )

    for p in range(PAIRS):
        for q in range(2):
            mixed = jnp.concatenate(
                [
                    jnp.concatenate([vb[part(p, odd, q), pl.ds((B + x) * PITCH + B, B), :] for x in range(B)], 0)
                    for odd in range(2)
                ],
                1,
            )
            natural = spread(mixed, join[...], 2)
            for h in range(2):
                f = p + h * PAIRS
                f1[f, q] = f1[f, q] + natural[:, h * NZ : (h + 1) * NZ].reshape(B, B, NZ)

    def untransform(x, c):
        total = [[f1[f, q, x] for q in range(2)] for f in range(SLOTS)]
        spectrum = [(total[0][0], None)] + [tuple(v) for v in total[1:]] + [(total[0][1], None)]
        values = irdft(spectrum, STEPS)
        for t in range(STEPS):
            obuf[t, x] = values[t]
        return c

    lax.fori_loop(0, B, untransform, 0)
    t4 = []
    for k in range(1, STEPS):
        d = (s + k) % STEPS
        copy = remote(obuf.at[d], out_ref.at[pl.ds(x0, B), pl.ds(y0, B)], t4s.at[k], t4r.at[s], step=d)
        copy.start()
        t4.append(copy)
    out_ref[pl.ds(x0, B), pl.ds(y0, B), :] = obuf[s]

    for copy in t1 + t2:
        copy.wait_send()
    pl.when(jnp.logical_not(active))(to_partner.wait_send)
    to_next.wait_send()
    for copy in halo:
        copy.wait_send()

    @pl.when(active)
    def _():
        for k in range(1, STEPS):
            d = (s + k) % STEPS
            remote(ee.at[block], epart.at[slot], rss.at[k], rsr.at[slot], step=d).wait_send()
            remote(
                uu.at[1, :, pl.ds(0, B), pl.ds(0, B)], f1.at[slot], t3s.at[k], t3r.at[slot], step=d
            ).wait_send()

    for k in range(1, STEPS):
        d = (s + k) % STEPS
        dx, dy = origin(d)
        remote(obuf.at[d], out_ref.at[pl.ds(dx, B), pl.ds(dy, B)], t4s.at[k], t4r.at[d], step=d).wait_recv()
    for copy in t4:
        copy.wait_send()


def per_device(initial_state, source, absorption):
    grid = (NX, NY, NZ)
    vmem = lambda *shape: pltpu.VMEM(shape, F32)
    dma = lambda n: pltpu.SemaphoreType.DMA((n,))
    result = pl.pallas_call(
        kernel,
        out_shape=pltpu.VMEM(grid, F32),
        in_specs=[pl.BlockSpec(memory_space=pl.ANY)] * 3,
        out_specs=pl.BlockSpec(memory_space=pltpu.VMEM),
        scratch_shapes=[
            vmem(*grid),
            vmem(*grid),
            vmem(B, B, NZ),
            vmem(STEPS, B, B, NZ),
            vmem(SLOTS, 2, B, B, NZ),
            vmem(2, NX, NY + 8, NZ),
            vmem(4, NX, NY + 8, NZ),
            vmem(2, 2, NX + 4, NY + 24, NZ),
            vmem(*grid),
            vmem(SLOTS, B, B, NZ),
            vmem(B, B, NZ),
            vmem(B, B, NZ),
            vmem(3 * B, 4 * B, NZ),
            vmem(16, 3 * B * PITCH + 8, NZ),
            vmem(16, 3 * B * PITCH + 8, NZ),
            vmem(24, 3 * B * PITCH + 8, NZ),
            pltpu.VMEM((2 * NZ, 2 * NZ), BF16),
            vmem(SLOTS, 2, B, B, NZ),
            vmem(STEPS, B, B, NZ),
            dma(3),
            dma(STEPS), dma(STEPS),
            dma(SLOTS), dma(STEPS),
            dma(STEPS), dma(SLOTS),
            dma(1), dma(1),
            dma(8), dma(8),
            dma(STEPS), dma(SLOTS),
            dma(STEPS), dma(STEPS),
        ],
        compiler_params=pltpu.CompilerParams(
            collective_id=0, has_side_effects=True, vmem_limit_bytes=60 * 2**20
        ),
        name="windows",
    )(source[0, 0], initial_state, absorption)
    moment = lax.axis_index("step").astype(F32)
    return (result * (GAMMA ** (-moment) / STEPS))[None, None]


def solution(mesh):
    return jax.shard_map(
        per_device,
        mesh=mesh,
        in_specs=(P(), P("win", "step", None, None, None), P()),
        out_specs=P("win", "step", None, None, None),
        check_vma=False,
    )
```

```python
import functools
import math

import jax
import jax.numpy as jnp
from jax import lax
from jax.experimental import pallas as pl
from jax.experimental.pallas import tpu as pltpu
from jax.sharding import PartitionSpec as P

SWEEPS = 8
STEPS = 16
WINDOWS = 8
SLOTS = 8
PAIRS = 4
PITCH = 32
ALPHA = 0.1
COUPLING = 0.05
GAMMA = ALPHA ** (1.0 / STEPS)
NX, NY, NZ = 32, 32, 128
B = 8
MESH = pl.DeviceIdType.MESH
F32 = jnp.float32
BF16 = jnp.bfloat16
HALF = NZ // 2


def hops(d):
    return min(d[0], 4 - d[0]) + min(d[1], 4 - d[1])


OFFSETS = [(i, j) for i in (2, 1, 3, 0) for j in (2, 1, 3, 0) if (i, j) != (0, 0)]
OFFSETS.sort(key=lambda d: -hops(d))
EVEN = [d for d in OFFSETS if sum(d) % 2 == 0]
ODD = [d for d in OFFSETS if sum(d) % 2 == 1]
PARTS = 2
PB = B // PARTS


def wpow(n, k):
    angle = 2.0 * math.pi * k / n
    return math.cos(angle), -math.sin(angle)


def times(c, s, re, im):
    if abs(s) < 1e-12:
        return (re, im) if c > 0 else (-re, None if im is None else -im)
    if abs(c) < 1e-12:
        if im is None:
            return None, (re if s > 0 else -re)
        return (-im, re) if s > 0 else (im, -re)
    if im is None:
        return c * re, s * re
    if abs(abs(c) - abs(s)) < 1e-12:
        h = abs(c)
        a, b = (re if c > 0 else -re), (im if c > 0 else -im)
        if c * s > 0:
            return h * (a - b), h * (b + a)
        return h * (a + b), h * (b - a)
    return c * re - s * im, c * im + s * re


def plus(a, b):
    return b if a is None else a if b is None else a + b


def minus(a, b):
    if b is None:
        return a
    return -b if a is None else a - b


def rdft(values):
    n = len(values)
    if n == 1:
        return [(values[0], None)]
    half = n // 2
    even, odd = rdft(values[0::2]), rdft(values[1::2])
    out = []
    for k in range(half + 1):
        if k == half:
            out.append((even[0][0] - odd[0][0], None))
            break
        if k <= half // 2:
            e, o = even[k], odd[k]
        else:
            e, o = even[half - k], odd[half - k]
            e = (e[0], None if e[1] is None else -e[1])
            o = (o[0], None if o[1] is None else -o[1])
        o = times(*wpow(n, k), *o)
        out.append((plus(e[0], o[0]), plus(e[1], o[1])))
    return out


def irdft(spectrum, n):
    if n == 1:
        return [spectrum[0][0]]
    half = n // 2
    even, odd = [], []
    for k in range(half // 2 + 1):
        x = spectrum[k]
        y = spectrum[half - k]
        ym = None if y[1] is None else -y[1]
        e = (plus(x[0], y[0]), plus(x[1], ym))
        d = (minus(x[0], y[0]), minus(x[1], ym))
        c, s = wpow(n, k)
        if 2 * k == half and half > 1:
            e = (x[0] + x[0], None)
            d = (None, x[1] + x[1])
        o = d if k == 0 else times_any(c, -s, *d)
        if k == 0 or 2 * k == half:
            e, o = (e[0], None), (o[0], None)
        even.append(e)
        odd.append(o)
    if half == 1:
        even, odd = even[:1], odd[:1]
    a, b = irdft(even, half), irdft(odd, half)
    out = [None] * n
    out[0::2], out[1::2] = a, b
    return out


def times_any(c, s, re, im):
    if re is None:
        r, i = times(c, s, im, None)
        return (None if i is None else -i), r
    return times(c, s, re, im)


def part(p, odd, q):
    return p * 4 + odd * 2 + q


def kz(odd):
    return 16 + odd


def dz(odd):
    return 18 + odd


def dd(odd):
    return 24 + odd


def spread(v, pick, terms=3):
    total = None
    for k in range(terms):
        part = v.astype(BF16)
        product = jnp.dot(part, pick, preferred_element_type=F32)
        total = product if total is None else total + product
        if k < terms - 1:
            v = v - part.astype(F32)
    return total


def table(values, index):
    out = jnp.float32(values[0])
    for k in range(1, len(values)):
        out = jnp.where(index == k, jnp.float32(values[k]), out)
    return out


def kernel(
    src_hbm, init_hbm, abs_hbm, out_ref,
    src, ab, init, tbuf, sbuf, spec, kc, uu, ee, epart, ends, before, dext, va, vb, kk, join, f1, obuf,
    lsem, t1s, t1r, t2s, t2r, rss, rsr, wns, wnr, has, har, t3s, t3r, t4s, t4r,
):
    s = lax.axis_index("step")
    w = lax.axis_index("win")
    bx, by = s // 4, s % 4
    core = w % 2
    x0 = pl.multiple_of(bx * B, B)
    y0 = pl.multiple_of(by * B, B)
    slot = s // 2
    active = (bx + by + core) % 2 == 0

    def slot_device(f):
        return 2 * f + (f // 2 + core) % 2

    def origin(d):
        return pl.multiple_of((d // 4) * B, B), pl.multiple_of((d % 4) * B, B)

    def remote(source, target, send, recv, step=None, win=None):
        return pltpu.make_async_remote_copy(
            source, target, send, recv,
            device_id={"step": s if step is None else step, "win": w if win is None else win},
            device_id_type=MESH,
        )

    def device(shift):
        return (bx + shift[0]) % 4 * 4 + (by + shift[1]) % 4

    load_src = pltpu.make_async_copy(src_hbm, src, lsem.at[0])
    load_abs = pltpu.make_async_copy(abs_hbm, ab, lsem.at[1])
    load_init = pltpu.make_async_copy(init_hbm.at[pl.ds(x0, B), pl.ds(y0, B)], init, lsem.at[2])
    load_src.start()
    load_abs.start()
    load_init.start()

    barrier = pltpu.get_barrier_semaphore()
    for k in range(1, STEPS):
        pl.semaphore_signal(barrier, inc=1, device_id={"step": (s + k) % STEPS, "win": w}, device_id_type=MESH)
    for k in (1, WINDOWS - 1):
        pl.semaphore_signal(barrier, inc=1, device_id={"step": s, "win": (w + k) % WINDOWS}, device_id_type=MESH)
    pl.semaphore_wait(barrier, STEPS - 1 + 2)
    load_src.wait()

    t1 = []
    for h in range(PARTS):
        for k, shift in enumerate(OFFSETS):
            d = device(shift)
            dx, dy = origin(d)
            copy = remote(
                src.at[pl.ds(dx + h * PB, PB), pl.ds(dy, B)], tbuf.at[s, pl.ds(h * PB, PB)],
                t1s.at[k, h], t1r.at[s, h], step=d,
            )
            copy.start()
            t1.append(copy)
    load_init.wait()
    load_abs.wait()
    tbuf[s] = src[pl.ds(x0, B), pl.ds(y0, B), :]

    cos_of = [math.cos(2 * math.pi * f / STEPS) for f in range(SLOTS)]
    sin_of = [math.sin(2 * math.pi * f / STEPS) for f in range(SLOTS)]
    c1 = table(cos_of, slot)
    c2 = table([-1.0] + cos_of[1:], slot)
    sn = table([0.0] + sin_of[1:], slot)

    def coefficients(a, cos1, cos2, sin):
        base = a + (1.0 + 6.0 * COUPLING)
        r1 = base - GAMMA * cos1
        im = GAMMA * sin
        scale1 = COUPLING / (r1 * r1 + im * im)
        r2 = base - GAMMA * cos2
        scale2 = COUPLING / (r2 * r2 + im * im)
        return r1 * scale1, r2 * scale2, -im * scale1

    @pl.when(active)
    def _():
        def plane(x, c):
            k1, k2, kb = coefficients(ab[x], c1, c2, sn)
            for n, value in enumerate((k1, k2, kb)):
                kc[n, x, pl.ds(0, NY), :] = value
            return c

        lax.fori_loop(0, NX, plane, 0, unroll=4)
        zero = jnp.zeros((NY + 24, NZ), F32)
        zrow = jnp.zeros((8, NZ), F32)
        for p in range(2):
            for c in range(2):
                uu[p, c, 0] = zero
                uu[p, c, NX + 1] = zero

        def rows(x, c):
            for p in range(2):
                for q in range(2):
                    uu[p, q, x, pl.ds(0, 8), :] = zrow
                    uu[p, q, x, pl.ds(40, 8), :] = zrow
            return c

        lax.fori_loop(1, NX + 1, rows, 0, unroll=4)

    first_window = jnp.where(w == 0, jnp.float32(1.0), jnp.float32(0.0))

    def transform(x, c):
        values = []
        for t in range(STEPS):
            v = tbuf[t, x]
            if t == 0:
                v = v + first_window * init[x]
            values.append(v * (GAMMA**t / COUPLING))
        out = rdft(values)
        sbuf[0, 0, x], sbuf[0, 1, x] = out[0][0], out[8][0]
        for f in range(1, SLOTS):
            sbuf[f, 0, x], sbuf[f, 1, x] = out[f]
        return c

    def to_slot(k, h, shift):
        d = device(shift)
        half = pl.ds(x0 + h * PB, PB)
        return remote(
            sbuf.at[d // 2, :, pl.ds(h * PB, PB)], spec.at[:, half, pl.ds(y0, B)],
            t2s.at[k, h], t2r.at[s, h], step=d,
        )

    def send_to_slots(act):
        def run(h):
            @pl.when(active)
            def _():
                for k, shift in enumerate(EVEN):
                    act(to_slot(k, h, shift))

            @pl.when(jnp.logical_not(active))
            def _():
                for k, shift in enumerate(ODD):
                    act(to_slot(k, h, shift))

        return run

    for h in range(PARTS):
        for k in range(1, STEPS):
            d = (s - k) % STEPS
            remote(
                src.at[pl.ds(0, PB), pl.ds(0, B)], tbuf.at[d, pl.ds(h * PB, PB)], t1s.at[0, h], t1r.at[d, h], step=d
            ).wait_recv()
        lax.fori_loop(h * PB, (h + 1) * PB, transform, 0)
        send_to_slots(lambda copy: copy.start())(h)

    wide_lane = lax.broadcasted_iota(jnp.int32, (3 * B, NZ), 1)
    low = wide_lane < HALF
    pick_z = lax.broadcasted_iota(jnp.int32, (NZ, 2 * NZ), 0)
    pick_l = lax.broadcasted_iota(jnp.int32, (NZ, 2 * NZ), 1)
    pick = jnp.where(pick_z == 2 * (pick_l % HALF) + pick_l // NZ, 1.0, 0.0).astype(BF16)
    join_r = lax.broadcasted_iota(jnp.int32, (2 * NZ, 2 * NZ), 0)
    join_c = lax.broadcasted_iota(jnp.int32, (2 * NZ, 2 * NZ), 1)
    goes = ((join_r // HALF) % 2) * NZ + 2 * (join_r % HALF) + join_r // NZ
    join[...] = jnp.where(join_c == goes, 1.0, 0.0).astype(BF16)

    def at(a, b):
        return jnp.where(low, jnp.float32(a), jnp.float32(b))

    def turned(v, odd):
        lanes = wide_lane[: v.shape[0]] % HALF
        if odd:
            return jnp.where(lanes == 0, 0.0, pltpu.roll(v, 1, 1))
        return jnp.where(lanes == HALF - 1, 0.0, pltpu.roll(v, NZ - 1, 1))

    def wide_plane(i, c):
        gx = x0 - B + i
        inx = jnp.logical_and(gx >= 0, gx < NX)
        gxc = jnp.clip(gx, 0, NX - 1)
        tiles, keeps = [], []
        for b in range(3):
            gy = by - 1 + b
            inside = jnp.logical_and(inx, jnp.logical_and(gy >= 0, gy < 4))
            keep = jnp.where(inside, jnp.float32(COUPLING), jnp.float32(0.0))
            tiles.append(ab[gxc, pl.ds(pl.multiple_of(jnp.clip(gy, 0, 3) * B, B), B), :])
            keeps.append(jnp.full((B, NZ), keep, F32))
        both = spread(jnp.concatenate(tiles, 0), pick)
        keep = jnp.concatenate(keeps, 0)
        rows = pl.ds(pl.multiple_of(i * PITCH, PITCH), 3 * B)
        for odd in range(2):
            base = both[:, odd * NZ : (odd + 1) * NZ] + (1.0 + 6.0 * COUPLING)
            for p in range(PAIRS):
                q = p + PAIRS
                r = base - at(GAMMA * cos_of[p], GAMMA * cos_of[q])
                im = at(GAMMA * sin_of[p], GAMMA * sin_of[q])
                scale = keep / (r * r + im * im)
                ka, kb = r * scale, -im * scale
                if p == 0:
                    r2 = base - at(-GAMMA, GAMMA * cos_of[q])
                    k2 = r2 * (keep / (r2 * r2 + im * im))
                    kk[kz(odd), rows, :] = k2
                kk[part(p, odd, 0), rows, :], kk[part(p, odd, 1), rows, :] = ka, kb
                if p == 2:
                    kk[4 + kz(odd), rows, :], kk[4 + dz(odd), rows, :] = ka, jnp.zeros_like(ka)
        return c

    lax.fori_loop(1, 3 * B - 1, wide_plane, 0)

    @pl.when(active)
    def _():
        for c in range(2):
            spec[c, pl.ds(x0, B), pl.ds(y0, B), :] = sbuf[slot, c]
        for shift in reversed(OFFSETS):
            d = device(shift)
            dx, dy = origin(d)
            for h in range(PARTS):
                remote(
                    sbuf.at[slot, :, pl.ds(0, PB)], spec.at[:, pl.ds(dx + h * PB, PB), pl.ds(dy, B)],
                    t2s.at[0, h], t2r.at[d, h], step=d,
                ).wait_recv()

    lane = lax.broadcasted_iota(jnp.int32, (8, NZ), 1)

    def z_sum(v):
        n = v.shape[0]
        at = jnp.concatenate([lane] * (n // 8), 0) if n > 8 else lane
        below = jnp.where(at == 0, 0.0, pltpu.roll(v, 1, 1))
        above = jnp.where(at == NZ - 1, 0.0, pltpu.roll(v, NZ - 1, 1))
        return below + above

    def neighbours(load, x, y, n):
        total = load(x - 1, y, n) + load(x + 1, y, n)
        total = total + (load(x, y - 1, n) + load(x, y + 1, n))
        return total + z_sum(load(x, y, n))

    p_end = 2.0 / (16 * GAMMA**15)
    ends_re = table([0.5 * p_end] + [p_end * v for v in cos_of[1:]], slot)
    ends_im = table([-0.5 * p_end] + [p_end * v for v in sin_of[1:]], slot)

    @pl.when(active)
    def _():
        def start(x, c):
            k1, k2, kb = (kc[n, x, pl.ds(0, NY), :] for n in range(3))
            s0, s1 = (spec[n, x, pl.ds(0, NY), :] for n in range(2))
            uu[0, 0, x + 1, pl.ds(8, NY), :] = k1 * s0 - kb * s1
            uu[0, 1, x + 1, pl.ds(8, NY), :] = k2 * s1 + kb * s0
            return c

        lax.fori_loop(0, NX, start, 0, unroll=4)

        def sweep(k, c):
            old = k % 2
            for x in range(NX):
                nb = [
                    neighbours(
                        lambda px, py, n, q=q: uu[old, q, px, pl.ds(py, n), :], x + 1, 8, NY
                    )
                    for q in range(2)
                ]
                k1, k2, kb = (kc[n, x, pl.ds(0, NY), :] for n in range(3))
                s0, s1 = (spec[n, x, pl.ds(0, NY), :] + nb[n] for n in range(2))
                uu[1 - old, 0, x + 1, pl.ds(8, NY), :] = k1 * s0 - kb * s1
                uu[1 - old, 1, x + 1, pl.ds(8, NY), :] = k2 * s1 + kb * s0
            return c

        lax.fori_loop(0, SWEEPS - 1, sweep, 0)

        def end(x, c):
            rows = pl.ds(8, NY)
            ee[x] = ends_re * uu[1, 0, x + 1, rows, :] + ends_im * uu[1, 1, x + 1, rows, :]
            return c

        lax.fori_loop(0, NX, end, 0, unroll=4)

        for k, shift in enumerate(OFFSETS):
            d = device(shift)
            dx, dy = origin(d)
            remote(ee.at[pl.ds(dx, B), pl.ds(dy, B)], epart.at[slot], rss.at[k], rsr.at[slot], step=d).start()
        epart[slot] = ee[pl.ds(x0, B), pl.ds(y0, B), :]

    partner = s + 1 - 2 * (s % 2)

    def slots_wait(wait):
        for k in range(1, SLOTS):
            f = (slot + k) % SLOTS
            wait(f, slot_device(f))
        pl.when(jnp.logical_not(active))(lambda: wait(slot, partner))

    block = (pl.ds(0, B), pl.ds(0, B))
    slots_wait(lambda f, d: remote(ee.at[block], epart.at[f], rss.at[0], rsr.at[f], step=d).wait_recv())
    for x in range(B):
        total = epart[0, x]
        for f in range(1, SLOTS):
            total = total + epart[f, x]
        ends[x] = total

    to_next = remote(ends, before, wns.at[0], wnr.at[0], win=(w + 1) % WINDOWS)
    to_next.start()
    to_next.wait_recv()
    later_window = jnp.where(w == 0, jnp.float32(0.0), jnp.float32(1.0 / COUPLING))
    change = later_window * before[...] - (ALPHA / COUPLING) * ends[...]
    pack = jnp.where(
        pick_z[:, :NZ] == 2 * (pick_l[:, :NZ] % HALF) + pick_l[:, :NZ] // HALF, 1.0, 0.0
    ).astype(BF16)
    dext[pl.ds(B, B), pl.ds(B, B), :] = spread(change.reshape(B * B, NZ), pack).reshape(B, B, NZ)

    shifts = [(i, j) for i in (-1, 0, 1) for j in (-1, 0, 1) if (i, j) != (0, 0)]
    centre = dext.at[pl.ds(B, B), pl.ds(B, B)]
    halo = []
    for k, (i, j) in enumerate(shifts):
        d = ((bx + i + 4) % 4) * 4 + (by + j + 4) % 4
        copy = remote(
            centre, dext.at[pl.ds(B - B * i, B), pl.ds(B - B * j, B)], has.at[k], har.at[k], step=d
        )
        copy.start()
        halo.append(copy)

    for copy in halo:
        copy.wait_recv()

    @pl.when(active)
    def _():
        for k, shift in enumerate(OFFSETS):
            d = device(shift)
            dx, dy = origin(d)
            remote(
                uu.at[1, :, pl.ds(dx + 1, B), pl.ds(pl.multiple_of(dy + 8, 8), B)],
                f1.at[slot], t3s.at[k], t3r.at[slot], step=d,
            ).start()
        for c in range(2):
            f1[slot, c] = uu[1, c, pl.ds(x0 + 1, B), pl.ds(pl.multiple_of(y0 + 8, 8), B), :]


    def wide_start(i, c):
        rows = pl.ds(pl.multiple_of(i * PITCH, PITCH), 3 * B)
        v = dext[i, pl.ds(0, 3 * B), :]
        swapped = pltpu.roll(v, HALF, 1)
        d = [jnp.where(low, v, swapped), jnp.where(low, swapped, v)]
        for odd in range(2):
            kk[dd(odd), rows, :] = d[odd]
            kk[dz(odd), rows, :] = jnp.where(low, d[odd], 0.0)
            for p in range(PAIRS):
                second = kk[part(p, odd, 1), rows, :]
                if p == 0:
                    second = jnp.where(low, kk[kz(odd), rows, :], second)
                va[part(p, odd, 0), rows, :] = kk[part(p, odd, 0), rows, :] * d[odd]
                va[part(p, odd, 1), rows, :] = second * d[odd]
        return c

    lax.fori_loop(1, 3 * B - 1, wide_start, 0)
    zero_row = s // STEPS
    for k in range(SWEEPS - 1):
        reach = SWEEPS - 2 - k
        vo, vn = (va, vb) if k % 2 == 0 else (vb, va)
        places = []
        for i in range(B - reach, 2 * B + reach):
            rest = reach - max(B - i, i - 2 * B + 1, 0)
            places += [i * PITCH + B - rest + 8 * tile for tile in range(-(-(B + 2 * rest) // 8))]

        def wide(g, c, vo=vo, vn=vn, places=places):
            for place in places:
                start = place + zero_row
                rows = pl.ds(start, 8)
                around = [pl.ds(start + shift, 8) for shift in (-PITCH, PITCH, -1, 1)]
                for p in range(2):
                    first = 8 * g
                    middle = [[vo[first + part(p, odd, q), rows, :] for q in range(2)] for odd in range(2)]
                    for odd in range(2):
                        nb = []
                        for q in range(2):
                            here, other = first + part(p, odd, q), middle[1 - odd][q]
                            t = vo[here, around[0], :] + vo[here, around[1], :]
                            t = t + (vo[here, around[2], :] + vo[here, around[3], :])
                            nb.append((t + other) + turned(other, 1 - odd))
                        ka, kb = kk[first + part(p, odd, 0), rows, :], kk[first + part(p, odd, 1), rows, :]
                        s0, s1, k2 = kk[dd(odd), rows, :] + nb[0], nb[1], ka
                        if p == 0:
                            s1, k2 = s1 + kk[4 * g + dz(odd), rows, :], kk[4 * g + kz(odd), rows, :]
                        vn[first + part(p, odd, 0), rows, :] = ka * s0 - kb * s1
                        vn[first + part(p, odd, 1), rows, :] = k2 * s1 + kb * s0
            return c

        lax.fori_loop(0, 2, wide, 0)

    slots_wait(
        lambda f, d: remote(uu.at[1, :, pl.ds(0, B), pl.ds(0, B)], f1.at[f], t3s.at[0], t3r.at[f], step=d).wait_recv()
    )

    for p in range(PAIRS):
        for q in range(2):
            mixed = jnp.concatenate(
                [
                    jnp.concatenate([vb[part(p, odd, q), pl.ds((B + x) * PITCH + B, B), :] for x in range(B)], 0)
                    for odd in range(2)
                ],
                1,
            )
            natural = spread(mixed, join[...], 2)
            for h in range(2):
                f = p + h * PAIRS
                f1[f, q] = f1[f, q] + natural[:, h * NZ : (h + 1) * NZ].reshape(B, B, NZ)

    def untransform(x, c):
        total = [[f1[f, q, x] for q in range(2)] for f in range(SLOTS)]
        spectrum = [(total[0][0], None)] + [tuple(v) for v in total[1:]] + [(total[0][1], None)]
        values = irdft(spectrum, STEPS)
        for t in range(STEPS):
            obuf[t, x] = values[t]
        return c

    lax.fori_loop(0, B, untransform, 0)
    t4 = []
    for k, shift in enumerate(OFFSETS):
        d = device(shift)
        copy = remote(obuf.at[d], out_ref.at[pl.ds(x0, B), pl.ds(y0, B)], t4s.at[k], t4r.at[s], step=d)
        copy.start()
        t4.append(copy)
    out_ref[pl.ds(x0, B), pl.ds(y0, B), :] = obuf[s]

    for copy in t1:
        copy.wait_send()
    for h in range(PARTS):
        send_to_slots(lambda copy: copy.wait_send())(h)
    to_next.wait_send()
    for copy in halo:
        copy.wait_send()

    @pl.when(active)
    def _():
        for k, shift in enumerate(OFFSETS):
            d = device(shift)
            remote(ee.at[block], epart.at[slot], rss.at[k], rsr.at[slot], step=d).wait_send()
            remote(
                uu.at[1, :, pl.ds(0, B), pl.ds(0, B)], f1.at[slot], t3s.at[k], t3r.at[slot], step=d
            ).wait_send()

    for k in range(1, STEPS):
        d = (s + k) % STEPS
        dx, dy = origin(d)
        remote(obuf.at[d], out_ref.at[pl.ds(dx, B), pl.ds(dy, B)], t4s.at[k], t4r.at[d], step=d).wait_recv()
    for copy in t4:
        copy.wait_send()


def per_device(initial_state, source, absorption):
    grid = (NX, NY, NZ)
    vmem = lambda *shape: pltpu.VMEM(shape, F32)
    dma = lambda *n: pltpu.SemaphoreType.DMA(n)
    result = pl.pallas_call(
        kernel,
        out_shape=pltpu.VMEM(grid, F32),
        in_specs=[pl.BlockSpec(memory_space=pl.ANY)] * 3,
        out_specs=pl.BlockSpec(memory_space=pltpu.VMEM),
        scratch_shapes=[
            vmem(*grid),
            vmem(*grid),
            vmem(B, B, NZ),
            vmem(STEPS, B, B, NZ),
            vmem(SLOTS, 2, B, B, NZ),
            vmem(2, NX, NY + 8, NZ),
            vmem(4, NX, NY + 8, NZ),
            vmem(2, 2, NX + 4, NY + 24, NZ),
            vmem(*grid),
            vmem(SLOTS, B, B, NZ),
            vmem(B, B, NZ),
            vmem(B, B, NZ),
            vmem(3 * B, 4 * B, NZ),
            vmem(16, 3 * B * PITCH + 8, NZ),
            vmem(16, 3 * B * PITCH + 8, NZ),
            vmem(28, 3 * B * PITCH + 8, NZ),
            pltpu.VMEM((2 * NZ, 2 * NZ), BF16),
            vmem(SLOTS, 2, B, B, NZ),
            vmem(STEPS, B, B, NZ),
            dma(3),
            dma(STEPS, PARTS), dma(STEPS, PARTS),
            dma(SLOTS, PARTS), dma(STEPS, PARTS),
            dma(STEPS), dma(SLOTS),
            dma(1), dma(1),
            dma(8), dma(8),
            dma(STEPS), dma(SLOTS),
            dma(STEPS), dma(STEPS),
        ],
        compiler_params=pltpu.CompilerParams(
            collective_id=0, has_side_effects=True, vmem_limit_bytes=60 * 2**20
        ),
        name="windows",
    )(source[0, 0], initial_state, absorption)
    moment = lax.axis_index("step").astype(F32)
    return (result * (GAMMA ** (-moment) / STEPS))[None, None]


def solution(mesh):
    return jax.shard_map(
        per_device,
        mesh=mesh,
        in_specs=(P(), P("win", "step", None, None, None), P()),
        out_specs=P("win", "step", None, None, None),
        check_vma=False,
    )
```

```python
import functools
import math

import jax
import jax.numpy as jnp
from jax import lax
from jax.experimental import pallas as pl
from jax.experimental.pallas import tpu as pltpu
from jax.sharding import PartitionSpec as P

SWEEPS = 8
STEPS = 16
WINDOWS = 8
SLOTS = 8
PAIRS = 4
PITCH = 32
ALPHA = 0.1
COUPLING = 0.05
GAMMA = ALPHA ** (1.0 / STEPS)
NX, NY, NZ = 32, 32, 128
B = 8
MESH = pl.DeviceIdType.MESH
F32 = jnp.float32
BF16 = jnp.bfloat16
HALF = NZ // 2


def hops(d):
    return min(d[0], 4 - d[0]) + min(d[1], 4 - d[1])


OFFSETS = [(i, j) for i in (2, 1, 3, 0) for j in (2, 1, 3, 0) if (i, j) != (0, 0)]
OFFSETS.sort(key=lambda d: -hops(d))
EVEN = [d for d in OFFSETS if sum(d) % 2 == 0]
ODD = [d for d in OFFSETS if sum(d) % 2 == 1]
PARTS = 2
PB = B // PARTS


def wpow(n, k):
    angle = 2.0 * math.pi * k / n
    return math.cos(angle), -math.sin(angle)


def times(c, s, re, im):
    if abs(s) < 1e-12:
        return (re, im) if c > 0 else (-re, None if im is None else -im)
    if abs(c) < 1e-12:
        if im is None:
            return None, (re if s > 0 else -re)
        return (-im, re) if s > 0 else (im, -re)
    if im is None:
        return c * re, s * re
    if abs(abs(c) - abs(s)) < 1e-12:
        h = abs(c)
        a, b = (re if c > 0 else -re), (im if c > 0 else -im)
        if c * s > 0:
            return h * (a - b), h * (b + a)
        return h * (a + b), h * (b - a)
    return c * re - s * im, c * im + s * re


def plus(a, b):
    return b if a is None else a if b is None else a + b


def minus(a, b):
    if b is None:
        return a
    return -b if a is None else a - b


def rdft(values):
    n = len(values)
    if n == 1:
        return [(values[0], None)]
    half = n // 2
    even, odd = rdft(values[0::2]), rdft(values[1::2])
    out = []
    for k in range(half + 1):
        if k == half:
            out.append((even[0][0] - odd[0][0], None))
            break
        if k <= half // 2:
            e, o = even[k], odd[k]
        else:
            e, o = even[half - k], odd[half - k]
            e = (e[0], None if e[1] is None else -e[1])
            o = (o[0], None if o[1] is None else -o[1])
        o = times(*wpow(n, k), *o)
        out.append((plus(e[0], o[0]), plus(e[1], o[1])))
    return out


def irdft(spectrum, n):
    if n == 1:
        return [spectrum[0][0]]
    half = n // 2
    even, odd = [], []
    for k in range(half // 2 + 1):
        x = spectrum[k]
        y = spectrum[half - k]
        ym = None if y[1] is None else -y[1]
        e = (plus(x[0], y[0]), plus(x[1], ym))
        d = (minus(x[0], y[0]), minus(x[1], ym))
        c, s = wpow(n, k)
        if 2 * k == half and half > 1:
            e = (x[0] + x[0], None)
            d = (None, x[1] + x[1])
        o = d if k == 0 else times_any(c, -s, *d)
        if k == 0 or 2 * k == half:
            e, o = (e[0], None), (o[0], None)
        even.append(e)
        odd.append(o)
    if half == 1:
        even, odd = even[:1], odd[:1]
    a, b = irdft(even, half), irdft(odd, half)
    out = [None] * n
    out[0::2], out[1::2] = a, b
    return out


def times_any(c, s, re, im):
    if re is None:
        r, i = times(c, s, im, None)
        return (None if i is None else -i), r
    return times(c, s, re, im)


def part(p, odd, q):
    return p * 4 + odd * 2 + q


def kz(odd):
    return 16 + odd


def dz(odd):
    return 18 + odd


def dd(odd):
    return 24 + odd


def spread(v, pick, terms=3):
    total = None
    for k in range(terms):
        part = v.astype(BF16)
        product = jnp.dot(part, pick, preferred_element_type=F32)
        total = product if total is None else total + product
        if k < terms - 1:
            v = v - part.astype(F32)
    return total


def table(values, index):
    out = jnp.float32(values[0])
    for k in range(1, len(values)):
        out = jnp.where(index == k, jnp.float32(values[k]), out)
    return out


def kernel(
    src_hbm, init_hbm, abs_hbm, out_ref,
    src, ab, init, tbuf, sbuf, spec, kc, uu, ee, epart, ends, before, dext, va, vb, kk, join, back, f1, obuf,
    lsem, t1s, t1r, t2s, t2r, rss, rsr, wns, wnr, has, har, t3s, t3r, t4s, t4r,
):
    s = lax.axis_index("step")
    w = lax.axis_index("win")
    bx, by = s // 4, s % 4
    core = w % 2
    x0 = pl.multiple_of(bx * B, B)
    y0 = pl.multiple_of(by * B, B)
    slot = s // 2
    active = (bx + by + core) % 2 == 0

    def slot_device(f):
        return 2 * f + (f // 2 + core) % 2

    def origin(d):
        return pl.multiple_of((d // 4) * B, B), pl.multiple_of((d % 4) * B, B)

    def remote(source, target, send, recv, step=None, win=None):
        return pltpu.make_async_remote_copy(
            source, target, send, recv,
            device_id={"step": s if step is None else step, "win": w if win is None else win},
            device_id_type=MESH,
        )

    def device(shift):
        return (bx + shift[0]) % 4 * 4 + (by + shift[1]) % 4

    load_src = pltpu.make_async_copy(src_hbm, src, lsem.at[0])
    load_abs = pltpu.make_async_copy(abs_hbm, ab, lsem.at[1])
    load_init = pltpu.make_async_copy(init_hbm.at[pl.ds(x0, B), pl.ds(y0, B)], init, lsem.at[2])
    load_src.start()
    load_abs.start()
    load_init.start()

    barrier = pltpu.get_barrier_semaphore()
    for k in range(1, STEPS):
        pl.semaphore_signal(barrier, inc=1, device_id={"step": (s + k) % STEPS, "win": w}, device_id_type=MESH)
    for k in (1, WINDOWS - 1):
        pl.semaphore_signal(barrier, inc=1, device_id={"step": s, "win": (w + k) % WINDOWS}, device_id_type=MESH)
    pl.semaphore_wait(barrier, STEPS - 1 + 2)
    load_src.wait()

    t1 = []
    for h in range(PARTS):
        for k, shift in enumerate(OFFSETS):
            d = device(shift)
            dx, dy = origin(d)
            copy = remote(
                src.at[pl.ds(dx + h * PB, PB), pl.ds(dy, B)], tbuf.at[s, pl.ds(h * PB, PB)],
                t1s.at[k, h], t1r.at[s, h], step=d,
            )
            copy.start()
            t1.append(copy)
    load_init.wait()
    load_abs.wait()
    tbuf[s] = src[pl.ds(x0, B), pl.ds(y0, B), :]

    cos_of = [math.cos(2 * math.pi * f / STEPS) for f in range(SLOTS)]
    sin_of = [math.sin(2 * math.pi * f / STEPS) for f in range(SLOTS)]
    c1 = table(cos_of, slot)
    c2 = table([-1.0] + cos_of[1:], slot)
    sn = table([0.0] + sin_of[1:], slot)

    def coefficients(a, cos1, cos2, sin):
        base = a + (1.0 + 6.0 * COUPLING)
        r1 = base - GAMMA * cos1
        im = GAMMA * sin
        scale1 = COUPLING / (r1 * r1 + im * im)
        r2 = base - GAMMA * cos2
        scale2 = COUPLING / (r2 * r2 + im * im)
        return r1 * scale1, r2 * scale2, -im * scale1

    @pl.when(active)
    def _():
        def plane(x, c):
            k1, k2, kb = coefficients(ab[x], c1, c2, sn)
            for n, value in enumerate((k1, k2, kb)):
                kc[n, x, pl.ds(0, NY), :] = value
            return c

        lax.fori_loop(0, NX, plane, 0, unroll=4)
        zero = jnp.zeros((NY + 24, NZ), F32)
        zrow = jnp.zeros((8, NZ), F32)
        for p in range(2):
            for c in range(2):
                uu[p, c, 0] = zero
                uu[p, c, NX + 1] = zero

        def rows(x, c):
            for p in range(2):
                for q in range(2):
                    uu[p, q, x, pl.ds(0, 8), :] = zrow
                    uu[p, q, x, pl.ds(40, 8), :] = zrow
            return c

        lax.fori_loop(1, NX + 1, rows, 0, unroll=4)

    first_window = jnp.where(w == 0, jnp.float32(1.0), jnp.float32(0.0))

    def transform(x, c):
        values = []
        for t in range(STEPS):
            v = tbuf[t, x]
            if t == 0:
                v = v + first_window * init[x]
            values.append(v * (GAMMA**t / COUPLING))
        out = rdft(values)
        sbuf[0, 0, x], sbuf[0, 1, x] = out[0][0], out[8][0]
        for f in range(1, SLOTS):
            sbuf[f, 0, x], sbuf[f, 1, x] = out[f]
        return c

    def to_slot(k, h, shift):
        d = device(shift)
        half = pl.ds(x0 + h * PB, PB)
        return remote(
            sbuf.at[d // 2, :, pl.ds(h * PB, PB)], spec.at[:, half, pl.ds(y0, B)],
            t2s.at[k, h], t2r.at[s, h], step=d,
        )

    def send_to_slots(act):
        def run(h):
            @pl.when(active)
            def _():
                for k, shift in enumerate(EVEN):
                    act(to_slot(k, h, shift))

            @pl.when(jnp.logical_not(active))
            def _():
                for k, shift in enumerate(ODD):
                    act(to_slot(k, h, shift))

        return run

    for h in range(PARTS):
        for k in range(1, STEPS):
            d = (s - k) % STEPS
            remote(
                src.at[pl.ds(0, PB), pl.ds(0, B)], tbuf.at[d, pl.ds(h * PB, PB)], t1s.at[0, h], t1r.at[d, h], step=d
            ).wait_recv()
        lax.fori_loop(h * PB, (h + 1) * PB, transform, 0)
        send_to_slots(lambda copy: copy.start())(h)

    wide_lane = lax.broadcasted_iota(jnp.int32, (3 * B, NZ), 1)
    low = wide_lane < HALF
    pick_z = lax.broadcasted_iota(jnp.int32, (NZ, 2 * NZ), 0)
    pick_l = lax.broadcasted_iota(jnp.int32, (NZ, 2 * NZ), 1)
    pick = jnp.where(pick_z == 2 * (pick_l % HALF) + pick_l // NZ, 1.0, 0.0).astype(BF16)
    join_r = lax.broadcasted_iota(jnp.int32, (2 * NZ, 2 * NZ), 0)
    join_c = lax.broadcasted_iota(jnp.int32, (2 * NZ, 2 * NZ), 1)
    goes = ((join_r // HALF) % 2) * NZ + 2 * (join_r % HALF) + join_r // NZ
    join[...] = jnp.where(join_c == goes, 1.0, 0.0).astype(BF16)

    def at(a, b):
        return jnp.where(low, jnp.float32(a), jnp.float32(b))

    def turned(v, odd):
        lanes = wide_lane[: v.shape[0]] % HALF
        if odd:
            return jnp.where(lanes == 0, 0.0, pltpu.roll(v, 1, 1))
        return jnp.where(lanes == HALF - 1, 0.0, pltpu.roll(v, NZ - 1, 1))

    def wide_plane(i, c):
        gx = x0 - B + i
        inx = jnp.logical_and(gx >= 0, gx < NX)
        gxc = jnp.clip(gx, 0, NX - 1)
        tiles, keeps = [], []
        for b in range(3):
            gy = by - 1 + b
            inside = jnp.logical_and(inx, jnp.logical_and(gy >= 0, gy < 4))
            keep = jnp.where(inside, jnp.float32(COUPLING), jnp.float32(0.0))
            tiles.append(ab[gxc, pl.ds(pl.multiple_of(jnp.clip(gy, 0, 3) * B, B), B), :])
            keeps.append(jnp.full((B, NZ), keep, F32))
        both = spread(jnp.concatenate(tiles, 0), pick)
        keep = jnp.concatenate(keeps, 0)
        rows = pl.ds(pl.multiple_of(i * PITCH, PITCH), 3 * B)
        for odd in range(2):
            base = both[:, odd * NZ : (odd + 1) * NZ] + (1.0 + 6.0 * COUPLING)
            for p in range(PAIRS):
                q = p + PAIRS
                r = base - at(GAMMA * cos_of[p], GAMMA * cos_of[q])
                im = at(GAMMA * sin_of[p], GAMMA * sin_of[q])
                scale = keep / (r * r + im * im)
                ka, kb = r * scale, -im * scale
                if p == 0:
                    r2 = base - at(-GAMMA, GAMMA * cos_of[q])
                    k2 = r2 * (keep / (r2 * r2 + im * im))
                    kk[kz(odd), rows, :] = k2
                kk[part(p, odd, 0), rows, :], kk[part(p, odd, 1), rows, :] = ka, kb
                if p == 2:
                    kk[4 + kz(odd), rows, :], kk[4 + dz(odd), rows, :] = ka, jnp.zeros_like(ka)
        return c

    lax.fori_loop(1, 3 * B - 1, wide_plane, 0)

    @pl.when(active)
    def _():
        def begin(dx, dy, count):
            rows = pl.ds(dy, B)
            for m in range(count):
                k1, k2, kb = (kc[n, dx + m, rows, :] for n in range(3))
                s0, s1 = (spec[n, dx + m, rows, :] for n in range(2))
                inner = pl.ds(pl.multiple_of(dy + 8, 8), B)
                uu[0, 0, dx + m + 1, inner, :] = k1 * s0 - kb * s1
                uu[0, 1, dx + m + 1, inner, :] = k2 * s1 + kb * s0

        for c in range(2):
            spec[c, pl.ds(x0, B), pl.ds(y0, B), :] = sbuf[slot, c]
        begin(x0, y0, B)
        for h in range(PARTS):
            for shift in reversed(EVEN + ODD):
                d = device(shift)
                dx, dy = origin(d)
                remote(
                    sbuf.at[slot, :, pl.ds(0, PB)], spec.at[:, pl.ds(dx + h * PB, PB), pl.ds(dy, B)],
                    t2s.at[0, h], t2r.at[d, h], step=d,
                ).wait_recv()
                begin(dx + h * PB, dy, PB)

    lane = lax.broadcasted_iota(jnp.int32, (8, NZ), 1)

    def z_sum(v):
        n = v.shape[0]
        at = jnp.concatenate([lane] * (n // 8), 0) if n > 8 else lane
        below = jnp.where(at == 0, 0.0, pltpu.roll(v, 1, 1))
        above = jnp.where(at == NZ - 1, 0.0, pltpu.roll(v, NZ - 1, 1))
        return below + above

    p_end = 2.0 / (16 * GAMMA**15)
    ends_re = table([0.5 * p_end] + [p_end * v for v in cos_of[1:]], slot)
    ends_im = table([-0.5 * p_end] + [p_end * v for v in sin_of[1:]], slot)

    @pl.when(active)
    def _():
        def sweep(k, c):
            old = k % 2

            def load(q, px, py):
                return uu[old, q, px, pl.ds(py, NY), :]

            for x in range(NX):
                nb = []
                for q in range(2):
                    t = load(q, x, 8) + load(q, x + 2, 8)
                    t = t + (load(q, x + 1, 7) + load(q, x + 1, 9))
                    nb.append(t + z_sum(load(q, x + 1, 8)))
                k1, k2, kb = (kc[n, x, pl.ds(0, NY), :] for n in range(3))
                s0, s1 = (spec[n, x, pl.ds(0, NY), :] + nb[n] for n in range(2))
                uu[1 - old, 0, x + 1, pl.ds(8, NY), :] = k1 * s0 - kb * s1
                uu[1 - old, 1, x + 1, pl.ds(8, NY), :] = k2 * s1 + kb * s0
            return c

        lax.fori_loop(0, SWEEPS - 1, sweep, 0)

        def end(x, c):
            rows = pl.ds(8, NY)
            ee[x] = ends_re * uu[1, 0, x + 1, rows, :] + ends_im * uu[1, 1, x + 1, rows, :]
            return c

        lax.fori_loop(0, NX, end, 0, unroll=4)

        for k, shift in enumerate(OFFSETS):
            d = device(shift)
            dx, dy = origin(d)
            remote(ee.at[pl.ds(dx, B), pl.ds(dy, B)], epart.at[slot], rss.at[k], rsr.at[slot], step=d).start()
        epart[slot] = ee[pl.ds(x0, B), pl.ds(y0, B), :]

    partner = s + 1 - 2 * (s % 2)

    def slots_wait(wait):
        for k in range(1, SLOTS):
            f = (slot + k) % SLOTS
            wait(f, slot_device(f))
        pl.when(jnp.logical_not(active))(lambda: wait(slot, partner))

    block = (pl.ds(0, B), pl.ds(0, B))
    slots_wait(lambda f, d: remote(ee.at[block], epart.at[f], rss.at[0], rsr.at[f], step=d).wait_recv())
    for x in range(B):
        total = epart[0, x]
        for f in range(1, SLOTS):
            total = total + epart[f, x]
        ends[x] = total

    to_next = remote(ends, before, wns.at[0], wnr.at[0], win=(w + 1) % WINDOWS)
    to_next.start()
    def from_slot(k, h, shift):
        d = device(shift)
        dx, dy = origin(d)
        return remote(
            uu.at[1, :, pl.ds(dx + h * PB + 1, PB), pl.ds(pl.multiple_of(dy + 8, 8), B)],
            f1.at[slot, :, pl.ds(h * PB, PB)], t3s.at[k, h], t3r.at[slot, h], step=d,
        )

    def return_field(h):
        @pl.when(active)
        def _():
            for k, shift in enumerate(OFFSETS):
                from_slot(k, h, shift).start()
            for c in range(2):
                f1[slot, c, pl.ds(h * PB, PB)] = uu[
                    1, c, pl.ds(x0 + h * PB + 1, PB), pl.ds(pl.multiple_of(y0 + 8, 8), B), :
                ]

    return_field(0)
    to_next.wait_recv()
    later_window = jnp.where(w == 0, jnp.float32(0.0), jnp.float32(1.0 / COUPLING))
    change = later_window * before[...] - (ALPHA / COUPLING) * ends[...]
    pack = jnp.where(
        pick_z[:, :NZ] == 2 * (pick_l[:, :NZ] % HALF) + pick_l[:, :NZ] // HALF, 1.0, 0.0
    ).astype(BF16)
    dext[pl.ds(B, B), pl.ds(B, B), :] = spread(change.reshape(B * B, NZ), pack).reshape(B, B, NZ)

    shifts = [(0, 1), (0, -1), (1, 0), (-1, 0), (1, 1), (-1, -1), (1, -1), (-1, 1)]
    centre = dext.at[pl.ds(B, B), pl.ds(B, B)]
    halo = []
    for k, (i, j) in enumerate(shifts):
        d = ((bx + i + 4) % 4) * 4 + (by + j + 4) % 4
        copy = remote(
            centre, dext.at[pl.ds(B - B * i, B), pl.ds(B - B * j, B)], has.at[k], har.at[k], step=d
        )
        copy.start()
        halo.append(copy)

    def wide_start(i, j):
        row = B - B * j
        mask = low[:B]
        for plane in range(max(B - B * i, 1), min(2 * B - B * i, 3 * B - 1)):
            rows = pl.ds(plane * PITCH + row, B)
            v = dext[plane, pl.ds(row, B), :]
            swapped = pltpu.roll(v, HALF, 1)
            d = [jnp.where(mask, v, swapped), jnp.where(mask, swapped, v)]
            for odd in range(2):
                kk[dd(odd), rows, :] = d[odd]
                kk[dz(odd), rows, :] = jnp.where(mask, d[odd], 0.0)
                for p in range(PAIRS):
                    second = kk[part(p, odd, 1), rows, :]
                    if p == 0:
                        second = jnp.where(mask, kk[kz(odd), rows, :], second)
                    va[part(p, odd, 0), rows, :] = kk[part(p, odd, 0), rows, :] * d[odd]
                    va[part(p, odd, 1), rows, :] = second * d[odd]

    wide_start(0, 0)
    for k, (i, j) in enumerate(shifts):
        halo[k].wait_recv()
        wide_start(i, j)

    return_field(1)

    zero_row = s // STEPS
    for k in range(SWEEPS - 1):
        reach = SWEEPS - 2 - k
        vo, vn = (va, vb) if k % 2 == 0 else (vb, va)
        places = []
        for i in range(B - reach, 2 * B + reach):
            rest = reach - max(B - i, i - 2 * B + 1, 0)
            places += [i * PITCH + B - rest + 8 * tile for tile in range(-(-(B + 2 * rest) // 8))]

        def wide(g, c, vo=vo, vn=vn, places=places):
            for place in places:
                start = place + zero_row
                rows = pl.ds(start, 8)
                around = [pl.ds(start + shift, 8) for shift in (-PITCH, PITCH, -1, 1)]
                for p in range(2):
                    first = 8 * g
                    middle = [[vo[first + part(p, odd, q), rows, :] for q in range(2)] for odd in range(2)]
                    for odd in range(2):
                        nb = []
                        for q in range(2):
                            here, other = first + part(p, odd, q), middle[1 - odd][q]
                            t = vo[here, around[0], :] + vo[here, around[1], :]
                            t = t + (vo[here, around[2], :] + vo[here, around[3], :])
                            nb.append((t + other) + turned(other, 1 - odd))
                        ka, kb = kk[first + part(p, odd, 0), rows, :], kk[first + part(p, odd, 1), rows, :]
                        s0, s1, k2 = kk[dd(odd), rows, :] + nb[0], nb[1], ka
                        if p == 0:
                            s1, k2 = s1 + kk[4 * g + dz(odd), rows, :], kk[4 * g + kz(odd), rows, :]
                        vn[first + part(p, odd, 0), rows, :] = ka * s0 - kb * s1
                        vn[first + part(p, odd, 1), rows, :] = k2 * s1 + kb * s0
            return c

        lax.fori_loop(0, 2, wide, 0)

    def natural(h):
        mixed = []
        for p in range(PAIRS):
            for q in range(2):
                sides = [
                    jnp.concatenate(
                        [vb[part(p, odd, q), pl.ds((B + h * PB + x) * PITCH + B, B), :] for x in range(PB)], 0
                    )
                    for odd in range(2)
                ]
                mixed.append(jnp.concatenate(sides, 1))
        mixed = jnp.concatenate(mixed, 0)
        high = mixed.astype(BF16)
        rest = (mixed - high.astype(F32)).astype(BF16)
        n = mixed.shape[0]
        both = jnp.dot(jnp.concatenate([high, rest], 0), join[...], preferred_element_type=F32)
        back[...] = both[:n] + both[n:]

    def untransform(h):
        for x in range(PB):
            total = []
            for f in range(SLOTS):
                lanes = pl.ds(f // PAIRS * NZ, NZ)
                total.append(
                    [
                        f1[f, q, h * PB + x]
                        + back[pl.ds(((f % PAIRS * 2 + q) * PB + x) * B, B), lanes]
                        for q in range(2)
                    ]
                )
            spectrum = [(total[0][0], None)] + [tuple(v) for v in total[1:]] + [(total[0][1], None)]
            values = irdft(spectrum, STEPS)
            for t in range(STEPS):
                obuf[t, h * PB + x] = values[t]

    def to_step(k, h, shift):
        d = device(shift)
        return remote(
            obuf.at[d, pl.ds(h * PB, PB)], out_ref.at[pl.ds(x0 + h * PB, PB), pl.ds(y0, B)],
            t4s.at[k, h], t4r.at[s, h], step=d,
        )

    for h in range(PARTS):
        natural(h)
        slots_wait(
            lambda f, d: remote(
                uu.at[1, :, pl.ds(0, PB), pl.ds(0, B)], f1.at[f, :, pl.ds(h * PB, PB)],
                t3s.at[0, h], t3r.at[f, h], step=d,
            ).wait_recv()
        )
        untransform(h)
        for k, shift in enumerate(OFFSETS):
            to_step(k, h, shift).start()
        out_ref[pl.ds(x0 + h * PB, PB), pl.ds(y0, B), :] = obuf[s, pl.ds(h * PB, PB)]

    for copy in t1:
        copy.wait_send()
    for h in range(PARTS):
        send_to_slots(lambda copy: copy.wait_send())(h)
    to_next.wait_send()
    for copy in halo:
        copy.wait_send()

    @pl.when(active)
    def _():
        for k, shift in enumerate(OFFSETS):
            d = device(shift)
            remote(ee.at[block], epart.at[slot], rss.at[k], rsr.at[slot], step=d).wait_send()
            for h in range(PARTS):
                from_slot(k, h, shift).wait_send()

    for h in range(PARTS):
        for k in range(1, STEPS):
            d = (s + k) % STEPS
            dx, dy = origin(d)
            remote(
                obuf.at[d, pl.ds(0, PB)], out_ref.at[pl.ds(dx + h * PB, PB), pl.ds(dy, B)],
                t4s.at[0, h], t4r.at[d, h], step=d,
            ).wait_recv()
        for k, shift in enumerate(OFFSETS):
            to_step(k, h, shift).wait_send()


def per_device(initial_state, source, absorption):
    grid = (NX, NY, NZ)
    vmem = lambda *shape: pltpu.VMEM(shape, F32)
    dma = lambda *n: pltpu.SemaphoreType.DMA(n)
    result = pl.pallas_call(
        kernel,
        out_shape=pltpu.VMEM(grid, F32),
        in_specs=[pl.BlockSpec(memory_space=pl.ANY)] * 3,
        out_specs=pl.BlockSpec(memory_space=pltpu.VMEM),
        scratch_shapes=[
            vmem(*grid),
            vmem(*grid),
            vmem(B, B, NZ),
            vmem(STEPS, B, B, NZ),
            vmem(SLOTS, 2, B, B, NZ),
            vmem(2, NX, NY + 8, NZ),
            vmem(4, NX, NY + 8, NZ),
            vmem(2, 2, NX + 4, NY + 24, NZ),
            vmem(*grid),
            vmem(SLOTS, B, B, NZ),
            vmem(B, B, NZ),
            vmem(B, B, NZ),
            vmem(3 * B, 4 * B, NZ),
            vmem(16, 3 * B * PITCH + 8, NZ),
            vmem(16, 3 * B * PITCH + 8, NZ),
            vmem(28, 3 * B * PITCH + 8, NZ),
            pltpu.VMEM((2 * NZ, 2 * NZ), BF16),
            vmem(2 * PAIRS * PB * B, 2 * NZ),
            vmem(SLOTS, 2, B, B, NZ),
            vmem(STEPS, B, B, NZ),
            dma(3),
            dma(STEPS, PARTS), dma(STEPS, PARTS),
            dma(SLOTS, PARTS), dma(STEPS, PARTS),
            dma(STEPS), dma(SLOTS),
            dma(1), dma(1),
            dma(8), dma(8),
            dma(STEPS, PARTS), dma(SLOTS, PARTS),
            dma(STEPS, PARTS), dma(STEPS, PARTS),
        ],
        compiler_params=pltpu.CompilerParams(
            collective_id=0, has_side_effects=True, vmem_limit_bytes=60 * 2**20
        ),
        name="windows",
    )(source[0, 0], initial_state, absorption)
    moment = lax.axis_index("step").astype(F32)
    return (result * (GAMMA ** (-moment) / STEPS))[None, None]


def solution(mesh):
    return jax.shard_map(
        per_device,
        mesh=mesh,
        in_specs=(P(), P("win", "step", None, None, None), P()),
        out_specs=P("win", "step", None, None, None),
        check_vma=False,
    )
```

```python
import functools
import math

import jax
import jax.numpy as jnp
from jax import lax
from jax.experimental import pallas as pl
from jax.experimental.pallas import tpu as pltpu
from jax.sharding import PartitionSpec as P

SWEEPS = 8
STEPS = 16
WINDOWS = 8
SLOTS = 8
PAIRS = 4
PITCH = 32
ALPHA = 0.1
COUPLING = 0.05
GAMMA = ALPHA ** (1.0 / STEPS)
NX, NY, NZ = 32, 32, 128
B = 8
MESH = pl.DeviceIdType.MESH
F32 = jnp.float32
BF16 = jnp.bfloat16
HALF = NZ // 2


def hops(d):
    return min(d[0], 4 - d[0]) + min(d[1], 4 - d[1])


OFFSETS = [(i, j) for i in (2, 1, 3, 0) for j in (2, 1, 3, 0) if (i, j) != (0, 0)]
OFFSETS.sort(key=lambda d: -hops(d))
EVEN = [d for d in OFFSETS if sum(d) % 2 == 0]
ODD = [d for d in OFFSETS if sum(d) % 2 == 1]
PARTS = 2
PB = B // PARTS
PIECES = 2
PC = B // PIECES


def wpow(n, k):
    angle = 2.0 * math.pi * k / n
    return math.cos(angle), -math.sin(angle)


def times(c, s, re, im):
    if abs(s) < 1e-12:
        return (re, im) if c > 0 else (-re, None if im is None else -im)
    if abs(c) < 1e-12:
        if im is None:
            return None, (re if s > 0 else -re)
        return (-im, re) if s > 0 else (im, -re)
    if im is None:
        return c * re, s * re
    if abs(abs(c) - abs(s)) < 1e-12:
        h = abs(c)
        a, b = (re if c > 0 else -re), (im if c > 0 else -im)
        if c * s > 0:
            return h * (a - b), h * (b + a)
        return h * (a + b), h * (b - a)
    return c * re - s * im, c * im + s * re


def plus(a, b):
    return b if a is None else a if b is None else a + b


def minus(a, b):
    if b is None:
        return a
    return -b if a is None else a - b


def rdft(values):
    n = len(values)
    if n == 1:
        return [(values[0], None)]
    half = n // 2
    even, odd = rdft(values[0::2]), rdft(values[1::2])
    out = []
    for k in range(half + 1):
        if k == half:
            out.append((even[0][0] - odd[0][0], None))
            break
        if k <= half // 2:
            e, o = even[k], odd[k]
        else:
            e, o = even[half - k], odd[half - k]
            e = (e[0], None if e[1] is None else -e[1])
            o = (o[0], None if o[1] is None else -o[1])
        o = times(*wpow(n, k), *o)
        out.append((plus(e[0], o[0]), plus(e[1], o[1])))
    return out


def irdft(spectrum, n):
    if n == 1:
        return [spectrum[0][0]]
    half = n // 2
    even, odd = [], []
    for k in range(half // 2 + 1):
        x = spectrum[k]
        y = spectrum[half - k]
        ym = None if y[1] is None else -y[1]
        e = (plus(x[0], y[0]), plus(x[1], ym))
        d = (minus(x[0], y[0]), minus(x[1], ym))
        c, s = wpow(n, k)
        if 2 * k == half and half > 1:
            e = (x[0] + x[0], None)
            d = (None, x[1] + x[1])
        o = d if k == 0 else times_any(c, -s, *d)
        if k == 0 or 2 * k == half:
            e, o = (e[0], None), (o[0], None)
        even.append(e)
        odd.append(o)
    if half == 1:
        even, odd = even[:1], odd[:1]
    a, b = irdft(even, half), irdft(odd, half)
    out = [None] * n
    out[0::2], out[1::2] = a, b
    return out


def times_any(c, s, re, im):
    if re is None:
        r, i = times(c, s, im, None)
        return (None if i is None else -i), r
    return times(c, s, re, im)


def part(p, odd, q):
    return p * 4 + odd * 2 + q


def kz(odd):
    return 16 + odd


def dz(odd):
    return 18 + odd


def dd(odd):
    return 24 + odd


def spread(v, pick, terms=3):
    total = None
    for k in range(terms):
        part = v.astype(BF16)
        product = jnp.dot(part, pick, preferred_element_type=F32)
        total = product if total is None else total + product
        if k < terms - 1:
            v = v - part.astype(F32)
    return total


def table(values, index):
    out = jnp.float32(values[0])
    for k in range(1, len(values)):
        out = jnp.where(index == k, jnp.float32(values[k]), out)
    return out


def kernel(
    src_hbm, init_hbm, abs_hbm, out_ref,
    src, ab, init, tbuf, sbuf, spec, kc, uu, ee, epart, ends, before, dext, va, vb, kk, join, back, f1, obuf,
    lsem, t1s, t1r, t2s, t2r, rss, rsr, wns, wnr, has, har, t3s, t3r, t4s, t4r,
):
    s = lax.axis_index("step")
    w = lax.axis_index("win")
    bx, by = s // 4, s % 4
    core = w % 2
    x0 = pl.multiple_of(bx * B, B)
    y0 = pl.multiple_of(by * B, B)
    slot = s // 2
    active = (bx + by + core) % 2 == 0

    def slot_device(f):
        return 2 * f + (f // 2 + core) % 2

    def origin(d):
        return pl.multiple_of((d // 4) * B, B), pl.multiple_of((d % 4) * B, B)

    def remote(source, target, send, recv, step=None, win=None):
        return pltpu.make_async_remote_copy(
            source, target, send, recv,
            device_id={"step": s if step is None else step, "win": w if win is None else win},
            device_id_type=MESH,
        )

    def device(shift):
        return (bx + shift[0]) % 4 * 4 + (by + shift[1]) % 4

    def counted(messages, rows, send, recv):
        size = va.at[pl.ds(0, messages), pl.ds(0, rows)]
        return remote(size, size, send, recv, step=(s + 1) % STEPS)

    load_src = pltpu.make_async_copy(src_hbm, src, lsem.at[0])
    load_abs = pltpu.make_async_copy(abs_hbm, ab, lsem.at[1])
    load_init = pltpu.make_async_copy(init_hbm.at[pl.ds(x0, B), pl.ds(y0, B)], init, lsem.at[2])
    load_src.start()
    load_abs.start()
    load_init.start()

    barrier = pltpu.get_barrier_semaphore()
    for k in range(1, STEPS):
        pl.semaphore_signal(barrier, inc=1, device_id={"step": (s + k) % STEPS, "win": w}, device_id_type=MESH)
    for k in (1, WINDOWS - 1):
        pl.semaphore_signal(barrier, inc=1, device_id={"step": s, "win": (w + k) % WINDOWS}, device_id_type=MESH)
    pl.semaphore_wait(barrier, STEPS - 1 + 2)
    load_src.wait()

    for h in range(PIECES):
        for k, shift in enumerate(OFFSETS):
            d = device(shift)
            dx, dy = origin(d)
            copy = remote(
                src.at[pl.ds(dx + h * PC, PC), pl.ds(dy, B)], tbuf.at[s, pl.ds(h * PC, PC)],
                t1s.at[0], t1r.at[h], step=d,
            )
            copy.start()
    load_init.wait()
    load_abs.wait()
    tbuf[s] = src[pl.ds(x0, B), pl.ds(y0, B), :]

    cos_of = [math.cos(2 * math.pi * f / STEPS) for f in range(SLOTS)]
    sin_of = [math.sin(2 * math.pi * f / STEPS) for f in range(SLOTS)]
    c1 = table(cos_of, slot)
    c2 = table([-1.0] + cos_of[1:], slot)
    sn = table([0.0] + sin_of[1:], slot)

    def coefficients(a, cos1, cos2, sin):
        base = a + (1.0 + 6.0 * COUPLING)
        r1 = base - GAMMA * cos1
        im = GAMMA * sin
        scale1 = COUPLING / (r1 * r1 + im * im)
        r2 = base - GAMMA * cos2
        scale2 = COUPLING / (r2 * r2 + im * im)
        return r1 * scale1, r2 * scale2, -im * scale1

    @pl.when(active)
    def _():
        def plane(x, c):
            k1, k2, kb = coefficients(ab[x], c1, c2, sn)
            for n, value in enumerate((k1, k2, kb)):
                kc[n, x, pl.ds(0, NY), :] = value
            return c

        lax.fori_loop(0, NX, plane, 0, unroll=4)
        zero = jnp.zeros((NY + 24, NZ), F32)
        zrow = jnp.zeros((8, NZ), F32)
        for p in range(2):
            for c in range(2):
                uu[p, c, 0] = zero
                uu[p, c, NX + 1] = zero

        def rows(x, c):
            for p in range(2):
                for q in range(2):
                    uu[p, q, x, pl.ds(0, 8), :] = zrow
                    uu[p, q, x, pl.ds(40, 8), :] = zrow
            return c

        lax.fori_loop(1, NX + 1, rows, 0, unroll=4)

    first_window = jnp.where(w == 0, jnp.float32(1.0), jnp.float32(0.0))

    def transform(x, c):
        values = []
        for t in range(STEPS):
            v = tbuf[t, x]
            if t == 0:
                v = v + first_window * init[x]
            values.append(v * (GAMMA**t / COUPLING))
        out = rdft(values)
        sbuf[0, 0, x], sbuf[0, 1, x] = out[0][0], out[8][0]
        for f in range(1, SLOTS):
            sbuf[f, 0, x], sbuf[f, 1, x] = out[f]
        return c

    def to_slot(k, h, shift):
        d = device(shift)
        half = pl.ds(x0 + h * PC, PC)
        return remote(
            sbuf.at[d // 2, :, pl.ds(h * PC, PC)], spec.at[:, half, pl.ds(y0, B)],
            t2s.at[0], t2r.at[h], step=d,
        )

    def send_to_slots(h):
        @pl.when(active)
        def _():
            for k, shift in enumerate(EVEN):
                to_slot(k, h, shift).start()

        @pl.when(jnp.logical_not(active))
        def _():
            for k, shift in enumerate(ODD):
                to_slot(k, h, shift).start()

    for h in range(PIECES):
        counted(STEPS - 1, PC * B, t1s.at[0], t1r.at[h]).wait_recv()
        lax.fori_loop(h * PC, (h + 1) * PC, transform, 0)
        send_to_slots(h)

    wide_lane = lax.broadcasted_iota(jnp.int32, (3 * B, NZ), 1)
    low = wide_lane < HALF
    pick_z = lax.broadcasted_iota(jnp.int32, (NZ, 2 * NZ), 0)
    pick_l = lax.broadcasted_iota(jnp.int32, (NZ, 2 * NZ), 1)
    pick = jnp.where(pick_z == 2 * (pick_l % HALF) + pick_l // NZ, 1.0, 0.0).astype(BF16)
    join_r = lax.broadcasted_iota(jnp.int32, (2 * NZ, 2 * NZ), 0)
    join_c = lax.broadcasted_iota(jnp.int32, (2 * NZ, 2 * NZ), 1)
    goes = ((join_r // HALF) % 2) * NZ + 2 * (join_r % HALF) + join_r // NZ
    join[...] = jnp.where(join_c == goes, 1.0, 0.0).astype(BF16)

    def at(a, b):
        return jnp.where(low, jnp.float32(a), jnp.float32(b))

    def turned(v, odd):
        lanes = wide_lane[: v.shape[0]] % HALF
        if odd:
            return jnp.where(lanes == 0, 0.0, pltpu.roll(v, 1, 1))
        return jnp.where(lanes == HALF - 1, 0.0, pltpu.roll(v, NZ - 1, 1))

    def wide_plane(i, c):
        gx = x0 - B + i
        inx = jnp.logical_and(gx >= 0, gx < NX)
        gxc = jnp.clip(gx, 0, NX - 1)
        tiles, keeps = [], []
        for b in range(3):
            gy = by - 1 + b
            inside = jnp.logical_and(inx, jnp.logical_and(gy >= 0, gy < 4))
            keep = jnp.where(inside, jnp.float32(COUPLING), jnp.float32(0.0))
            tiles.append(ab[gxc, pl.ds(pl.multiple_of(jnp.clip(gy, 0, 3) * B, B), B), :])
            keeps.append(jnp.full((B, NZ), keep, F32))
        both = spread(jnp.concatenate(tiles, 0), pick)
        keep = jnp.concatenate(keeps, 0)
        rows = pl.ds(pl.multiple_of(i * PITCH, PITCH), 3 * B)
        for odd in range(2):
            base = both[:, odd * NZ : (odd + 1) * NZ] + (1.0 + 6.0 * COUPLING)
            for p in range(PAIRS):
                q = p + PAIRS
                r = base - at(GAMMA * cos_of[p], GAMMA * cos_of[q])
                im = at(GAMMA * sin_of[p], GAMMA * sin_of[q])
                scale = keep / (r * r + im * im)
                ka, kb = r * scale, -im * scale
                if p == 0:
                    r2 = base - at(-GAMMA, GAMMA * cos_of[q])
                    k2 = r2 * (keep / (r2 * r2 + im * im))
                    kk[kz(odd), rows, :] = k2
                kk[part(p, odd, 0), rows, :], kk[part(p, odd, 1), rows, :] = ka, kb
                if p == 2:
                    kk[4 + kz(odd), rows, :], kk[4 + dz(odd), rows, :] = ka, jnp.zeros_like(ka)
        return c

    lax.fori_loop(1, 3 * B - 1, wide_plane, 0)

    @pl.when(active)
    def _():
        for c in range(2):
            spec[c, pl.ds(x0, B), pl.ds(y0, B), :] = sbuf[slot, c]
        for h in range(PIECES):
            counted(STEPS - 1, 2 * PC * B, t2s.at[0], t2r.at[h]).wait_recv()

            def begin(i, c, h=h):
                for m in range(PC):
                    x = i * B + h * PC + m
                    k1, k2, kb = (kc[n, x, pl.ds(0, NY), :] for n in range(3))
                    s0, s1 = (spec[n, x, pl.ds(0, NY), :] for n in range(2))
                    uu[0, 0, x + 1, pl.ds(8, NY), :] = k1 * s0 - kb * s1
                    uu[0, 1, x + 1, pl.ds(8, NY), :] = k2 * s1 + kb * s0
                return c

            lax.fori_loop(0, NX // B, begin, 0)

    lane = lax.broadcasted_iota(jnp.int32, (8, NZ), 1)

    def z_sum(v):
        n = v.shape[0]
        at = jnp.concatenate([lane] * (n // 8), 0) if n > 8 else lane
        below = jnp.where(at == 0, 0.0, pltpu.roll(v, 1, 1))
        above = jnp.where(at == NZ - 1, 0.0, pltpu.roll(v, NZ - 1, 1))
        return below + above

    p_end = 2.0 / (16 * GAMMA**15)
    ends_re = table([0.5 * p_end] + [p_end * v for v in cos_of[1:]], slot)
    ends_im = table([-0.5 * p_end] + [p_end * v for v in sin_of[1:]], slot)

    @pl.when(active)
    def _():
        def sweep(k, c):
            old = k % 2

            def load(q, px, py):
                return uu[old, q, px, pl.ds(py, NY), :]

            for x in range(NX):
                nb = []
                for q in range(2):
                    t = load(q, x, 8) + load(q, x + 2, 8)
                    t = t + (load(q, x + 1, 7) + load(q, x + 1, 9))
                    nb.append(t + z_sum(load(q, x + 1, 8)))
                k1, k2, kb = (kc[n, x, pl.ds(0, NY), :] for n in range(3))
                s0, s1 = (spec[n, x, pl.ds(0, NY), :] + nb[n] for n in range(2))
                uu[1 - old, 0, x + 1, pl.ds(8, NY), :] = k1 * s0 - kb * s1
                uu[1 - old, 1, x + 1, pl.ds(8, NY), :] = k2 * s1 + kb * s0
            return c

        lax.fori_loop(0, SWEEPS - 1, sweep, 0)

        def end(x, c):
            rows = pl.ds(8, NY)
            ee[x] = ends_re * uu[1, 0, x + 1, rows, :] + ends_im * uu[1, 1, x + 1, rows, :]
            return c

        lax.fori_loop(0, NX, end, 0, unroll=4)

        for k, shift in enumerate(OFFSETS):
            d = device(shift)
            dx, dy = origin(d)
            remote(ee.at[pl.ds(dx, B), pl.ds(dy, B)], epart.at[slot], rss.at[0], rsr.at[0], step=d).start()
        epart[slot] = ee[pl.ds(x0, B), pl.ds(y0, B), :]

    def slots_wait(rows, send, recv):
        pl.when(active)(lambda: counted(SLOTS - 1, rows, send, recv).wait_recv())
        pl.when(jnp.logical_not(active))(lambda: counted(SLOTS, rows, send, recv).wait_recv())

    slots_wait(B * B, rss.at[0], rsr.at[0])
    for x in range(B):
        total = epart[0, x]
        for f in range(1, SLOTS):
            total = total + epart[f, x]
        ends[x] = total

    to_next = remote(ends, before, wns.at[0], wnr.at[0], win=(w + 1) % WINDOWS)
    to_next.start()
    def from_slot(k, h, shift):
        d = device(shift)
        dx, dy = origin(d)
        return remote(
            uu.at[1, :, pl.ds(dx + h * PB + 1, PB), pl.ds(pl.multiple_of(dy + 8, 8), B)],
            f1.at[slot, :, pl.ds(h * PB, PB)], t3s.at[0], t3r.at[h], step=d,
        )

    def return_field(h):
        @pl.when(active)
        def _():
            for k, shift in enumerate(OFFSETS):
                from_slot(k, h, shift).start()
            for c in range(2):
                f1[slot, c, pl.ds(h * PB, PB)] = uu[
                    1, c, pl.ds(x0 + h * PB + 1, PB), pl.ds(pl.multiple_of(y0 + 8, 8), B), :
                ]

    return_field(0)
    to_next.wait_recv()
    later_window = jnp.where(w == 0, jnp.float32(0.0), jnp.float32(1.0 / COUPLING))
    change = later_window * before[...] - (ALPHA / COUPLING) * ends[...]
    pack = jnp.where(
        pick_z[:, :NZ] == 2 * (pick_l[:, :NZ] % HALF) + pick_l[:, :NZ] // HALF, 1.0, 0.0
    ).astype(BF16)
    dext[pl.ds(B, B), pl.ds(B, B), :] = spread(change.reshape(B * B, NZ), pack).reshape(B, B, NZ)

    shifts = [(0, 1), (0, -1), (1, 0), (-1, 0), (1, 1), (-1, -1), (1, -1), (-1, 1)]
    for k, (i, j) in enumerate(shifts):
        d = ((bx + i + 4) % 4) * 4 + (by + j + 4) % 4
        n = B - abs(i) * (1 + abs(j))
        first = B if i < 1 else 2 * B - n
        remote(
            dext.at[pl.ds(first, n), pl.ds(B, B)],
            dext.at[pl.ds(first - B * i, n), pl.ds(B - B * j, B)],
            has.at[0], har.at[k // 4], step=d,
        ).start()

    def wide_start(i, j):
        row = B - B * j
        mask = low[:B]
        n = B - abs(i) * (1 + abs(j))
        first = (B if i < 1 else 2 * B - n) - B * i
        for plane in range(first, first + n):
            rows = pl.ds(plane * PITCH + row, B)
            v = dext[plane, pl.ds(row, B), :]
            swapped = pltpu.roll(v, HALF, 1)
            d = [jnp.where(mask, v, swapped), jnp.where(mask, swapped, v)]
            for odd in range(2):
                kk[dd(odd), rows, :] = d[odd]
                kk[dz(odd), rows, :] = jnp.where(mask, d[odd], 0.0)
                for p in range(PAIRS):
                    second = kk[part(p, odd, 1), rows, :]
                    if p == 0:
                        second = jnp.where(mask, kk[kz(odd), rows, :], second)
                    va[part(p, odd, 0), rows, :] = kk[part(p, odd, 0), rows, :] * d[odd]
                    va[part(p, odd, 1), rows, :] = second * d[odd]

    wide_start(0, 0)
    for k in range(2):
        counted(4, (60, 48)[k], has.at[0], har.at[k]).wait_recv()
        for i, j in shifts[4 * k : 4 * k + 4]:
            wide_start(i, j)

    return_field(1)

    zero_row = s // STEPS
    for k in range(SWEEPS - 1):
        reach = SWEEPS - 2 - k
        vo, vn = (va, vb) if k % 2 == 0 else (vb, va)
        places = []
        for i in range(B - reach, 2 * B + reach):
            rest = reach - max(B - i, i - 2 * B + 1, 0)
            places += [i * PITCH + B - rest + 8 * tile for tile in range(-(-(B + 2 * rest) // 8))]

        def wide(g, c, vo=vo, vn=vn, places=places):
            for place in places:
                start = place + zero_row
                rows = pl.ds(start, 8)
                around = [pl.ds(start + shift, 8) for shift in (-PITCH, PITCH, -1, 1)]
                for p in range(2):
                    first = 8 * g
                    middle = [[vo[first + part(p, odd, q), rows, :] for q in range(2)] for odd in range(2)]
                    for odd in range(2):
                        nb = []
                        for q in range(2):
                            here, other = first + part(p, odd, q), middle[1 - odd][q]
                            t = vo[here, around[0], :] + vo[here, around[1], :]
                            t = t + (vo[here, around[2], :] + vo[here, around[3], :])
                            nb.append((t + other) + turned(other, 1 - odd))
                        ka, kb = kk[first + part(p, odd, 0), rows, :], kk[first + part(p, odd, 1), rows, :]
                        s0, s1, k2 = kk[dd(odd), rows, :] + nb[0], nb[1], ka
                        if p == 0:
                            s1, k2 = s1 + kk[4 * g + dz(odd), rows, :], kk[4 * g + kz(odd), rows, :]
                        vn[first + part(p, odd, 0), rows, :] = ka * s0 - kb * s1
                        vn[first + part(p, odd, 1), rows, :] = k2 * s1 + kb * s0
            return c

        lax.fori_loop(0, 2, wide, 0)

    def natural(h):
        mixed = []
        for p in range(PAIRS):
            for q in range(2):
                sides = [
                    jnp.concatenate(
                        [vb[part(p, odd, q), pl.ds((B + h * PB + x) * PITCH + B, B), :] for x in range(PB)], 0
                    )
                    for odd in range(2)
                ]
                mixed.append(jnp.concatenate(sides, 1))
        mixed = jnp.concatenate(mixed, 0)
        high = mixed.astype(BF16)
        rest = (mixed - high.astype(F32)).astype(BF16)
        n = mixed.shape[0]
        both = jnp.dot(jnp.concatenate([high, rest], 0), join[...], preferred_element_type=F32)
        back[...] = both[:n] + both[n:]

    def untransform(h):
        for x in range(PB):
            total = []
            for f in range(SLOTS):
                lanes = pl.ds(f // PAIRS * NZ, NZ)
                total.append(
                    [
                        f1[f, q, h * PB + x]
                        + back[pl.ds(((f % PAIRS * 2 + q) * PB + x) * B, B), lanes]
                        for q in range(2)
                    ]
                )
            spectrum = [(total[0][0], None)] + [tuple(v) for v in total[1:]] + [(total[0][1], None)]
            values = irdft(spectrum, STEPS)
            for t in range(STEPS):
                obuf[t, h * PB + x] = values[t]

    def to_step(k, h, shift):
        d = device(shift)
        return remote(
            obuf.at[d, pl.ds(h * PB, PB)], out_ref.at[pl.ds(x0 + h * PB, PB), pl.ds(y0, B)],
            t4s.at[0], t4r.at[0], step=d,
        )

    for h in range(PARTS):
        natural(h)
        slots_wait(2 * PB * B, t3s.at[0], t3r.at[h])
        untransform(h)
        for k, shift in enumerate(OFFSETS):
            to_step(k, h, shift).start()
        out_ref[pl.ds(x0 + h * PB, PB), pl.ds(y0, B), :] = obuf[s, pl.ds(h * PB, PB)]

    counted(STEPS - 1, B * B, t1s.at[0], t1r.at[0]).wait_send()
    to_next.wait_send()
    counted(8, 54, has.at[0], har.at[0]).wait_send()

    @pl.when(active)
    def _():
        counted(SLOTS - 1, 2 * B * B, t2s.at[0], t2r.at[0]).wait_send()
        counted(STEPS - 1, B * B, rss.at[0], rsr.at[0]).wait_send()
        counted(STEPS - 1, 2 * B * B, t3s.at[0], t3r.at[0]).wait_send()

    @pl.when(jnp.logical_not(active))
    def _():
        counted(SLOTS, 2 * B * B, t2s.at[0], t2r.at[0]).wait_send()

    last = counted(STEPS - 1, B * B, t4s.at[0], t4r.at[0])
    last.wait_send()
    last.wait_recv()


def per_device(initial_state, source, absorption):
    grid = (NX, NY, NZ)
    vmem = lambda *shape: pltpu.VMEM(shape, F32)
    dma = lambda *n: pltpu.SemaphoreType.DMA(n)
    result = pl.pallas_call(
        kernel,
        out_shape=pltpu.VMEM(grid, F32),
        in_specs=[pl.BlockSpec(memory_space=pl.ANY)] * 3,
        out_specs=pl.BlockSpec(memory_space=pltpu.VMEM),
        scratch_shapes=[
            vmem(*grid),
            vmem(*grid),
            vmem(B, B, NZ),
            vmem(STEPS, B, B, NZ),
            vmem(SLOTS, 2, B, B, NZ),
            vmem(2, NX, NY + 8, NZ),
            vmem(4, NX, NY + 8, NZ),
            vmem(2, 2, NX + 4, NY + 24, NZ),
            vmem(*grid),
            vmem(SLOTS, B, B, NZ),
            vmem(B, B, NZ),
            vmem(B, B, NZ),
            vmem(3 * B, 4 * B, NZ),
            vmem(16, 3 * B * PITCH + 8, NZ),
            vmem(16, 3 * B * PITCH + 8, NZ),
            vmem(28, 3 * B * PITCH + 8, NZ),
            pltpu.VMEM((2 * NZ, 2 * NZ), BF16),
            vmem(2 * PAIRS * PB * B, 2 * NZ),
            vmem(SLOTS, 2, B, B, NZ),
            vmem(STEPS, B, B, NZ),
            dma(3),
            dma(1), dma(PIECES),
            dma(1), dma(PIECES),
            dma(1), dma(1),
            dma(1), dma(1),
            dma(1), dma(2),
            dma(1), dma(PARTS),
            dma(1), dma(1),
        ],
        compiler_params=pltpu.CompilerParams(
            collective_id=0, has_side_effects=True, vmem_limit_bytes=60 * 2**20
        ),
        name="windows",
    )(source[0, 0], initial_state, absorption)
    moment = lax.axis_index("step").astype(F32)
    return (result * (GAMMA ** (-moment) / STEPS))[None, None]


def solution(mesh):
    return jax.shard_map(
        per_device,
        mesh=mesh,
        in_specs=(P(), P("win", "step", None, None, None), P()),
        out_specs=P("win", "step", None, None, None),
        check_vma=False,
    )
```

```python
import functools
import math

import jax
import jax.numpy as jnp
from jax import lax
from jax.experimental import pallas as pl
from jax.experimental.pallas import tpu as pltpu
from jax.sharding import PartitionSpec as P

SWEEPS = 8
STEPS = 16
WINDOWS = 8
SLOTS = 8
PAIRS = 4
PITCH = 32
ALPHA = 0.1
COUPLING = 0.05
GAMMA = ALPHA ** (1.0 / STEPS)
NX, NY, NZ = 32, 32, 128
B = 8
MESH = pl.DeviceIdType.MESH
F32 = jnp.float32
BF16 = jnp.bfloat16
HALF = NZ // 2


def hops(d):
    return min(d[0], 4 - d[0]) + min(d[1], 4 - d[1])


OFFSETS = [(i, j) for i in (2, 1, 3, 0) for j in (2, 1, 3, 0) if (i, j) != (0, 0)]
OFFSETS.sort(key=lambda d: -hops(d))
EVEN = [d for d in OFFSETS if sum(d) % 2 == 0]
ODD = [d for d in OFFSETS if sum(d) % 2 == 1]
PARTS = 2
PB = B // PARTS
PIECES = 2
PC = B // PIECES


def wpow(n, k):
    angle = 2.0 * math.pi * k / n
    return math.cos(angle), -math.sin(angle)


def times(c, s, re, im):
    if abs(s) < 1e-12:
        return (re, im) if c > 0 else (-re, None if im is None else -im)
    if abs(c) < 1e-12:
        if im is None:
            return None, (re if s > 0 else -re)
        return (-im, re) if s > 0 else (im, -re)
    if im is None:
        return c * re, s * re
    if abs(abs(c) - abs(s)) < 1e-12:
        h = abs(c)
        a, b = (re if c > 0 else -re), (im if c > 0 else -im)
        if c * s > 0:
            return h * (a - b), h * (b + a)
        return h * (a + b), h * (b - a)
    return c * re - s * im, c * im + s * re


def plus(a, b):
    return b if a is None else a if b is None else a + b


def minus(a, b):
    if b is None:
        return a
    return -b if a is None else a - b


def rdft(values):
    n = len(values)
    if n == 1:
        return [(values[0], None)]
    half = n // 2
    even, odd = rdft(values[0::2]), rdft(values[1::2])
    out = []
    for k in range(half + 1):
        if k == half:
            out.append((even[0][0] - odd[0][0], None))
            break
        if k <= half // 2:
            e, o = even[k], odd[k]
        else:
            e, o = even[half - k], odd[half - k]
            e = (e[0], None if e[1] is None else -e[1])
            o = (o[0], None if o[1] is None else -o[1])
        o = times(*wpow(n, k), *o)
        out.append((plus(e[0], o[0]), plus(e[1], o[1])))
    return out


def irdft(spectrum, n):
    if n == 1:
        return [spectrum[0][0]]
    half = n // 2
    even, odd = [], []
    for k in range(half // 2 + 1):
        x = spectrum[k]
        y = spectrum[half - k]
        ym = None if y[1] is None else -y[1]
        e = (plus(x[0], y[0]), plus(x[1], ym))
        d = (minus(x[0], y[0]), minus(x[1], ym))
        c, s = wpow(n, k)
        if 2 * k == half and half > 1:
            e = (x[0] + x[0], None)
            d = (None, x[1] + x[1])
        o = d if k == 0 else times_any(c, -s, *d)
        if k == 0 or 2 * k == half:
            e, o = (e[0], None), (o[0], None)
        even.append(e)
        odd.append(o)
    if half == 1:
        even, odd = even[:1], odd[:1]
    a, b = irdft(even, half), irdft(odd, half)
    out = [None] * n
    out[0::2], out[1::2] = a, b
    return out


def times_any(c, s, re, im):
    if re is None:
        r, i = times(c, s, im, None)
        return (None if i is None else -i), r
    return times(c, s, re, im)


def part(p, odd, q):
    return p * 4 + odd * 2 + q


def kz(odd):
    return 16 + odd


def dz(odd):
    return 18 + odd


def dd(odd):
    return 24 + odd


def spread(v, pick, terms=3):
    total = None
    for k in range(terms):
        part = v.astype(BF16)
        product = jnp.dot(part, pick, preferred_element_type=F32)
        total = product if total is None else total + product
        if k < terms - 1:
            v = v - part.astype(F32)
    return total


def table(values, index):
    out = jnp.float32(values[0])
    for k in range(1, len(values)):
        out = jnp.where(index == k, jnp.float32(values[k]), out)
    return out


def kernel(
    src_hbm, init_hbm, abs_hbm, out_ref,
    src, ab, init, tbuf, sbuf, spec, kc, uu, ee, epart, ends, before, dext, va, vb, kk, join, back, f1, obuf,
    lsem, t1s, t1r, t2s, t2r, rss, rsr, wns, wnr, has, har, t3s, t3r, t4s, t4r,
):
    s = lax.axis_index("step")
    w = lax.axis_index("win")
    bx, by = s // 4, s % 4
    core = w % 2
    x0 = pl.multiple_of(bx * B, B)
    y0 = pl.multiple_of(by * B, B)
    slot = s // 2
    active = (bx + by + core) % 2 == 0

    def slot_device(f):
        return 2 * f + (f // 2 + core) % 2

    def origin(d):
        return pl.multiple_of((d // 4) * B, B), pl.multiple_of((d % 4) * B, B)

    def remote(source, target, send, recv, step=None, win=None):
        return pltpu.make_async_remote_copy(
            source, target, send, recv,
            device_id={"step": s if step is None else step, "win": w if win is None else win},
            device_id_type=MESH,
        )

    def device(shift):
        return (bx + shift[0]) % 4 * 4 + (by + shift[1]) % 4

    def counted(messages, rows, send, recv):
        size = va.at[pl.ds(0, messages), pl.ds(0, rows)]
        return remote(size, size, send, recv, step=(s + 1) % STEPS)

    load_src = pltpu.make_async_copy(src_hbm, src, lsem.at[0])
    load_abs = pltpu.make_async_copy(abs_hbm, ab, lsem.at[1])
    load_init = pltpu.make_async_copy(init_hbm.at[pl.ds(x0, B), pl.ds(y0, B)], init, lsem.at[2])
    load_src.start()
    load_abs.start()
    load_init.start()

    barrier = pltpu.get_barrier_semaphore()
    for k in range(1, STEPS):
        pl.semaphore_signal(barrier, inc=1, device_id={"step": (s + k) % STEPS, "win": w}, device_id_type=MESH)
    for k in (1, WINDOWS - 1):
        pl.semaphore_signal(barrier, inc=1, device_id={"step": s, "win": (w + k) % WINDOWS}, device_id_type=MESH)
    pl.semaphore_wait(barrier, STEPS - 1 + 2)
    load_src.wait()

    for h in range(PIECES):
        for k, shift in enumerate(OFFSETS):
            d = device(shift)
            dx, dy = origin(d)
            copy = remote(
                src.at[pl.ds(dx + h * PC, PC), pl.ds(dy, B)], tbuf.at[s, pl.ds(h * PC, PC)],
                t1s.at[0], t1r.at[h], step=d,
            )
            copy.start()
    load_init.wait()
    load_abs.wait()
    tbuf[s] = src[pl.ds(x0, B), pl.ds(y0, B), :]

    cos_of = [math.cos(2 * math.pi * f / STEPS) for f in range(SLOTS)]
    sin_of = [math.sin(2 * math.pi * f / STEPS) for f in range(SLOTS)]
    c1 = table(cos_of, slot)
    c2 = table([-1.0] + cos_of[1:], slot)
    sn = table([0.0] + sin_of[1:], slot)

    def coefficients(a, cos1, cos2, sin):
        base = a + (1.0 + 6.0 * COUPLING)
        r1 = base - GAMMA * cos1
        im = GAMMA * sin
        scale1 = COUPLING / (r1 * r1 + im * im)
        r2 = base - GAMMA * cos2
        scale2 = COUPLING / (r2 * r2 + im * im)
        return r1 * scale1, r2 * scale2, -im * scale1

    @pl.when(active)
    def _():
        def plane(x, c):
            k1, k2, kb = coefficients(ab[x], c1, c2, sn)
            for n, value in enumerate((k1, k2, kb)):
                kc[n, x, pl.ds(0, NY), :] = value
            return c

        lax.fori_loop(0, NX, plane, 0, unroll=4)
        zero = jnp.zeros((NY + 24, NZ), F32)
        zrow = jnp.zeros((8, NZ), F32)
        for p in range(2):
            for c in range(2):
                uu[p, c, 0] = zero
                uu[p, c, NX + 1] = zero

        def rows(x, c):
            for p in range(2):
                for q in range(2):
                    uu[p, q, x, pl.ds(0, 8), :] = zrow
                    uu[p, q, x, pl.ds(40, 8), :] = zrow
            return c

        lax.fori_loop(1, NX + 1, rows, 0, unroll=4)

    first_window = jnp.where(w == 0, jnp.float32(1.0), jnp.float32(0.0))

    def transform(x, c):
        values = []
        for t in range(STEPS):
            v = tbuf[t, x]
            if t == 0:
                v = v + first_window * init[x]
            values.append(v * (GAMMA**t / COUPLING))
        out = rdft(values)
        sbuf[0, 0, x], sbuf[0, 1, x] = out[0][0], out[8][0]
        for f in range(1, SLOTS):
            sbuf[f, 0, x], sbuf[f, 1, x] = out[f]
        return c

    def to_slot(k, h, shift):
        d = device(shift)
        half = pl.ds(x0 + h * PC, PC)
        return remote(
            sbuf.at[d // 2, :, pl.ds(h * PC, PC)], spec.at[:, half, pl.ds(y0, B)],
            t2s.at[0], t2r.at[h], step=d,
        )

    def send_to_slots(h):
        @pl.when(active)
        def _():
            for k, shift in enumerate(EVEN):
                to_slot(k, h, shift).start()

        @pl.when(jnp.logical_not(active))
        def _():
            for k, shift in enumerate(ODD):
                to_slot(k, h, shift).start()

    for h in range(PIECES):
        counted(STEPS - 1, PC * B, t1s.at[0], t1r.at[h]).wait_recv()
        lax.fori_loop(h * PC, (h + 1) * PC, transform, 0)
        send_to_slots(h)

    wide_lane = lax.broadcasted_iota(jnp.int32, (3 * B, NZ), 1)
    low = wide_lane < HALF
    pick_z = lax.broadcasted_iota(jnp.int32, (NZ, 2 * NZ), 0)
    pick_l = lax.broadcasted_iota(jnp.int32, (NZ, 2 * NZ), 1)
    pick = jnp.where(pick_z == 2 * (pick_l % HALF) + pick_l // NZ, 1.0, 0.0).astype(BF16)
    join_r = lax.broadcasted_iota(jnp.int32, (2 * NZ, 2 * NZ), 0)
    join_c = lax.broadcasted_iota(jnp.int32, (2 * NZ, 2 * NZ), 1)
    goes = ((join_r // HALF) % 2) * NZ + 2 * (join_r % HALF) + join_r // NZ
    join[...] = jnp.where(join_c == goes, 1.0, 0.0).astype(BF16)

    def at(a, b):
        return jnp.where(low, jnp.float32(a), jnp.float32(b))

    def turned(v, odd):
        lanes = wide_lane[: v.shape[0]] % HALF
        if odd:
            return jnp.where(lanes == 0, 0.0, pltpu.roll(v, 1, 1))
        return jnp.where(lanes == HALF - 1, 0.0, pltpu.roll(v, NZ - 1, 1))

    def wide_plane(i, c):
        gx = x0 - B + i
        inx = jnp.logical_and(gx >= 0, gx < NX)
        gxc = jnp.clip(gx, 0, NX - 1)
        tiles, keeps = [], []
        for b in range(3):
            gy = by - 1 + b
            inside = jnp.logical_and(inx, jnp.logical_and(gy >= 0, gy < 4))
            keep = jnp.where(inside, jnp.float32(COUPLING), jnp.float32(0.0))
            tiles.append(ab[gxc, pl.ds(pl.multiple_of(jnp.clip(gy, 0, 3) * B, B), B), :])
            keeps.append(jnp.full((B, NZ), keep, F32))
        both = spread(jnp.concatenate(tiles, 0), pick)
        keep = jnp.concatenate(keeps, 0)
        rows = pl.ds(pl.multiple_of(i * PITCH, PITCH), 3 * B)
        for odd in range(2):
            base = both[:, odd * NZ : (odd + 1) * NZ] + (1.0 + 6.0 * COUPLING)
            for p in range(PAIRS):
                q = p + PAIRS
                r = base - at(GAMMA * cos_of[p], GAMMA * cos_of[q])
                im = at(GAMMA * sin_of[p], GAMMA * sin_of[q])
                scale = keep / (r * r + im * im)
                ka, kb = r * scale, -im * scale
                if p == 0:
                    r2 = base - at(-GAMMA, GAMMA * cos_of[q])
                    k2 = r2 * (keep / (r2 * r2 + im * im))
                    kk[kz(odd), rows, :] = k2
                kk[part(p, odd, 0), rows, :], kk[part(p, odd, 1), rows, :] = ka, kb
                if p == 2:
                    kk[4 + kz(odd), rows, :], kk[4 + dz(odd), rows, :] = ka, jnp.zeros_like(ka)
        return c

    lax.fori_loop(1, 3 * B - 1, wide_plane, 0)

    @pl.when(active)
    def _():
        for c in range(2):
            spec[c, pl.ds(x0, B), pl.ds(y0, B), :] = sbuf[slot, c]
        for h in range(PIECES):
            counted(STEPS - 1, 2 * PC * B, t2s.at[0], t2r.at[h]).wait_recv()

            def begin(i, c, h=h):
                for m in range(PC):
                    x = i * B + h * PC + m
                    k1, k2, kb = (kc[n, x, pl.ds(0, NY), :] for n in range(3))
                    s0, s1 = (spec[n, x, pl.ds(0, NY), :] for n in range(2))
                    uu[0, 0, x + 1, pl.ds(8, NY), :] = k1 * s0 - kb * s1
                    uu[0, 1, x + 1, pl.ds(8, NY), :] = k2 * s1 + kb * s0
                return c

            lax.fori_loop(0, NX // B, begin, 0)

    lane = lax.broadcasted_iota(jnp.int32, (8, NZ), 1)

    def z_sum(v):
        n = v.shape[0]
        at = jnp.concatenate([lane] * (n // 8), 0) if n > 8 else lane
        below = jnp.where(at == 0, 0.0, pltpu.roll(v, 1, 1))
        above = jnp.where(at == NZ - 1, 0.0, pltpu.roll(v, NZ - 1, 1))
        return below + above

    p_end = 2.0 / (16 * GAMMA**15)
    ends_re = table([0.5 * p_end] + [p_end * v for v in cos_of[1:]], slot)
    ends_im = table([-0.5 * p_end] + [p_end * v for v in sin_of[1:]], slot)

    @pl.when(active)
    def _():
        def sweep(k, c):
            old = k % 2

            def load(q, px, py):
                return uu[old, q, px, pl.ds(py, NY), :]

            for x in range(NX):
                nb = []
                for q in range(2):
                    t = load(q, x, 8) + load(q, x + 2, 8)
                    t = t + (load(q, x + 1, 7) + load(q, x + 1, 9))
                    nb.append(t + z_sum(load(q, x + 1, 8)))
                k1, k2, kb = (kc[n, x, pl.ds(0, NY), :] for n in range(3))
                s0, s1 = (spec[n, x, pl.ds(0, NY), :] + nb[n] for n in range(2))
                uu[1 - old, 0, x + 1, pl.ds(8, NY), :] = k1 * s0 - kb * s1
                uu[1 - old, 1, x + 1, pl.ds(8, NY), :] = k2 * s1 + kb * s0
            return c

        lax.fori_loop(0, SWEEPS - 1, sweep, 0)

        def end(x, c):
            rows = pl.ds(8, NY)
            ee[x] = ends_re * uu[1, 0, x + 1, rows, :] + ends_im * uu[1, 1, x + 1, rows, :]
            return c

        lax.fori_loop(0, NX, end, 0, unroll=4)

        for k, shift in enumerate(OFFSETS):
            d = device(shift)
            dx, dy = origin(d)
            remote(ee.at[pl.ds(dx, B), pl.ds(dy, B)], epart.at[slot], rss.at[0], rsr.at[0], step=d).start()
        epart[slot] = ee[pl.ds(x0, B), pl.ds(y0, B), :]

    def from_slot(k, h, shift):
        d = device(shift)
        dx, dy = origin(d)
        return remote(
            uu.at[1, :, pl.ds(dx + h * PB + 1, PB), pl.ds(pl.multiple_of(dy + 8, 8), B)],
            f1.at[slot, :, pl.ds(h * PB, PB)], t3s.at[0], t3r.at[h], step=d,
        )

    def return_field(h):
        @pl.when(active)
        def _():
            for k, shift in enumerate(OFFSETS):
                from_slot(k, h, shift).start()
            for c in range(2):
                f1[slot, c, pl.ds(h * PB, PB)] = uu[
                    1, c, pl.ds(x0 + h * PB + 1, PB), pl.ds(pl.multiple_of(y0 + 8, 8), B), :
                ]

    return_field(0)

    def slots_wait(rows, send, recv):
        pl.when(active)(lambda: counted(SLOTS - 1, rows, send, recv).wait_recv())
        pl.when(jnp.logical_not(active))(lambda: counted(SLOTS, rows, send, recv).wait_recv())

    slots_wait(B * B, rss.at[0], rsr.at[0])
    for x in range(B):
        total = epart[0, x]
        for f in range(1, SLOTS):
            total = total + epart[f, x]
        ends[x] = total

    to_next = remote(ends, before, wns.at[0], wnr.at[0], win=(w + 1) % WINDOWS)
    to_next.start()
    to_next.wait_recv()
    later_window = jnp.where(w == 0, jnp.float32(0.0), jnp.float32(1.0 / COUPLING))
    change = later_window * before[...] - (ALPHA / COUPLING) * ends[...]
    pack = jnp.where(
        pick_z[:, :NZ] == 2 * (pick_l[:, :NZ] % HALF) + pick_l[:, :NZ] // HALF, 1.0, 0.0
    ).astype(BF16)
    dext[pl.ds(B, B), pl.ds(B, B), :] = spread(change.reshape(B * B, NZ), pack).reshape(B, B, NZ)

    shifts = [(0, 1), (0, -1), (1, 0), (-1, 0), (1, 1), (-1, -1), (1, -1), (-1, 1)]
    for k, (i, j) in enumerate(shifts):
        d = ((bx + i + 4) % 4) * 4 + (by + j + 4) % 4
        n = B - abs(i) * (1 + abs(j))
        first = B if i < 1 else 2 * B - n
        remote(
            dext.at[pl.ds(first, n), pl.ds(B, B)],
            dext.at[pl.ds(first - B * i, n), pl.ds(B - B * j, B)],
            has.at[0], har.at[k // 4], step=d,
        ).start()

    def wide_start(i, j):
        row = B - B * j
        mask = low[:B]
        n = B - abs(i) * (1 + abs(j))
        first = (B if i < 1 else 2 * B - n) - B * i
        for plane in range(first, first + n):
            rows = pl.ds(plane * PITCH + row, B)
            v = dext[plane, pl.ds(row, B), :]
            swapped = pltpu.roll(v, HALF, 1)
            d = [jnp.where(mask, v, swapped), jnp.where(mask, swapped, v)]
            for odd in range(2):
                kk[dd(odd), rows, :] = d[odd]
                kk[dz(odd), rows, :] = jnp.where(mask, d[odd], 0.0)
                for p in range(PAIRS):
                    second = kk[part(p, odd, 1), rows, :]
                    if p == 0:
                        second = jnp.where(mask, kk[kz(odd), rows, :], second)
                    va[part(p, odd, 0), rows, :] = kk[part(p, odd, 0), rows, :] * d[odd]
                    va[part(p, odd, 1), rows, :] = second * d[odd]

    wide_start(0, 0)
    for k in range(2):
        counted(4, (60, 48)[k], has.at[0], har.at[k]).wait_recv()
        for i, j in shifts[4 * k : 4 * k + 4]:
            wide_start(i, j)

    return_field(1)

    zero_row = s // STEPS
    for k in range(SWEEPS - 1):
        reach = SWEEPS - 2 - k
        vo, vn = (va, vb) if k % 2 == 0 else (vb, va)
        places = []
        for i in range(B - reach, 2 * B + reach):
            rest = reach - max(B - i, i - 2 * B + 1, 0)
            places += [i * PITCH + B - rest + 8 * tile for tile in range(-(-(B + 2 * rest) // 8))]

        def wide(g, c, vo=vo, vn=vn, places=places):
            for place in places:
                start = place + zero_row
                rows = pl.ds(start, 8)
                around = [pl.ds(start + shift, 8) for shift in (-PITCH, PITCH, -1, 1)]
                for p in range(2):
                    first = 8 * g
                    middle = [[vo[first + part(p, odd, q), rows, :] for q in range(2)] for odd in range(2)]
                    for odd in range(2):
                        nb = []
                        for q in range(2):
                            here, other = first + part(p, odd, q), middle[1 - odd][q]
                            t = vo[here, around[0], :] + vo[here, around[1], :]
                            t = t + (vo[here, around[2], :] + vo[here, around[3], :])
                            nb.append((t + other) + turned(other, 1 - odd))
                        ka, kb = kk[first + part(p, odd, 0), rows, :], kk[first + part(p, odd, 1), rows, :]
                        s0, s1, k2 = kk[dd(odd), rows, :] + nb[0], nb[1], ka
                        if p == 0:
                            s1, k2 = s1 + kk[4 * g + dz(odd), rows, :], kk[4 * g + kz(odd), rows, :]
                        vn[first + part(p, odd, 0), rows, :] = ka * s0 - kb * s1
                        vn[first + part(p, odd, 1), rows, :] = k2 * s1 + kb * s0
            return c

        lax.fori_loop(0, 2, wide, 0)

    def natural(h):
        mixed = []
        for p in range(PAIRS):
            for q in range(2):
                sides = [
                    jnp.concatenate(
                        [vb[part(p, odd, q), pl.ds((B + h * PB + x) * PITCH + B, B), :] for x in range(PB)], 0
                    )
                    for odd in range(2)
                ]
                mixed.append(jnp.concatenate(sides, 1))
        mixed = jnp.concatenate(mixed, 0)
        high = mixed.astype(BF16)
        rest = (mixed - high.astype(F32)).astype(BF16)
        n = mixed.shape[0]
        both = jnp.dot(jnp.concatenate([high, rest], 0), join[...], preferred_element_type=F32)
        back[...] = both[:n] + both[n:]

    def untransform(h):
        for x in range(PB):
            total = []
            for f in range(SLOTS):
                lanes = pl.ds(f // PAIRS * NZ, NZ)
                total.append(
                    [
                        f1[f, q, h * PB + x]
                        + back[pl.ds(((f % PAIRS * 2 + q) * PB + x) * B, B), lanes]
                        for q in range(2)
                    ]
                )
            spectrum = [(total[0][0], None)] + [tuple(v) for v in total[1:]] + [(total[0][1], None)]
            values = irdft(spectrum, STEPS)
            for t in range(STEPS):
                obuf[t, h * PB + x] = values[t]

    def to_step(k, h, shift):
        d = device(shift)
        return remote(
            obuf.at[d, pl.ds(h * PB, PB)], out_ref.at[pl.ds(x0 + h * PB, PB), pl.ds(y0, B)],
            t4s.at[0], t4r.at[0], step=d,
        )

    for h in range(PARTS):
        natural(h)
        slots_wait(2 * PB * B, t3s.at[0], t3r.at[h])
        untransform(h)
        for k, shift in enumerate(OFFSETS):
            to_step(k, h, shift).start()
        out_ref[pl.ds(x0 + h * PB, PB), pl.ds(y0, B), :] = obuf[s, pl.ds(h * PB, PB)]

    counted(STEPS - 1, B * B, t1s.at[0], t1r.at[0]).wait_send()
    to_next.wait_send()
    counted(8, 54, has.at[0], har.at[0]).wait_send()

    @pl.when(active)
    def _():
        counted(SLOTS - 1, 2 * B * B, t2s.at[0], t2r.at[0]).wait_send()
        counted(STEPS - 1, B * B, rss.at[0], rsr.at[0]).wait_send()
        counted(STEPS - 1, 2 * B * B, t3s.at[0], t3r.at[0]).wait_send()

    @pl.when(jnp.logical_not(active))
    def _():
        counted(SLOTS, 2 * B * B, t2s.at[0], t2r.at[0]).wait_send()

    last = counted(STEPS - 1, B * B, t4s.at[0], t4r.at[0])
    last.wait_send()
    last.wait_recv()


def per_device(initial_state, source, absorption):
    grid = (NX, NY, NZ)
    vmem = lambda *shape: pltpu.VMEM(shape, F32)
    dma = lambda *n: pltpu.SemaphoreType.DMA(n)
    result = pl.pallas_call(
        kernel,
        out_shape=pltpu.VMEM(grid, F32),
        in_specs=[pl.BlockSpec(memory_space=pl.ANY)] * 3,
        out_specs=pl.BlockSpec(memory_space=pltpu.VMEM),
        scratch_shapes=[
            vmem(*grid),
            vmem(*grid),
            vmem(B, B, NZ),
            vmem(STEPS, B, B, NZ),
            vmem(SLOTS, 2, B, B, NZ),
            vmem(2, NX, NY + 8, NZ),
            vmem(4, NX, NY + 8, NZ),
            vmem(2, 2, NX + 4, NY + 24, NZ),
            vmem(*grid),
            vmem(SLOTS, B, B, NZ),
            vmem(B, B, NZ),
            vmem(B, B, NZ),
            vmem(3 * B, 4 * B, NZ),
            vmem(16, 3 * B * PITCH + 8, NZ),
            vmem(16, 3 * B * PITCH + 8, NZ),
            vmem(28, 3 * B * PITCH + 8, NZ),
            pltpu.VMEM((2 * NZ, 2 * NZ), BF16),
            vmem(2 * PAIRS * PB * B, 2 * NZ),
            vmem(SLOTS, 2, B, B, NZ),
            vmem(STEPS, B, B, NZ),
            dma(3),
            dma(1), dma(PIECES),
            dma(1), dma(PIECES),
            dma(1), dma(1),
            dma(1), dma(1),
            dma(1), dma(2),
            dma(1), dma(PARTS),
            dma(1), dma(1),
        ],
        compiler_params=pltpu.CompilerParams(
            collective_id=0, has_side_effects=True, vmem_limit_bytes=60 * 2**20
        ),
        name="windows",
    )(source[0, 0], initial_state, absorption)
    moment = lax.axis_index("step").astype(F32)
    return (result * (GAMMA ** (-moment) / STEPS))[None, None]


def solution(mesh):
    return jax.shard_map(
        per_device,
        mesh=mesh,
        in_specs=(P(), P("win", "step", None, None, None), P()),
        out_specs=P("win", "step", None, None, None),
        check_vma=False,
    )
```

```python
import functools
import math

import jax
import jax.numpy as jnp
from jax import lax
from jax.experimental import pallas as pl
from jax.experimental.pallas import tpu as pltpu
from jax.sharding import PartitionSpec as P

SWEEPS = 8
STEPS = 16
WINDOWS = 8
SLOTS = 8
PAIRS = 4
PITCH = 32
ALPHA = 0.1
COUPLING = 0.05
GAMMA = ALPHA ** (1.0 / STEPS)
NX, NY, NZ = 32, 32, 128
B = 8
MESH = pl.DeviceIdType.MESH
F32 = jnp.float32
BF16 = jnp.bfloat16
HALF = NZ // 2


def hops(d):
    return min(d[0], 4 - d[0]) + min(d[1], 4 - d[1])


OFFSETS = [(i, j) for i in (2, 1, 3, 0) for j in (2, 1, 3, 0) if (i, j) != (0, 0)]
OFFSETS.sort(key=lambda d: -hops(d))
EVEN = [d for d in OFFSETS if sum(d) % 2 == 0]
ODD = [d for d in OFFSETS if sum(d) % 2 == 1]
PARTS = 2
PB = B // PARTS
PIECES = 2
PC = B // PIECES
TURNS = 4
PT = B // TURNS


def wpow(n, k):
    angle = 2.0 * math.pi * k / n
    return math.cos(angle), -math.sin(angle)


def times(c, s, re, im):
    if abs(s) < 1e-12:
        return (re, im) if c > 0 else (-re, None if im is None else -im)
    if abs(c) < 1e-12:
        if im is None:
            return None, (re if s > 0 else -re)
        return (-im, re) if s > 0 else (im, -re)
    if im is None:
        return c * re, s * re
    if abs(abs(c) - abs(s)) < 1e-12:
        h = abs(c)
        a, b = (re if c > 0 else -re), (im if c > 0 else -im)
        if c * s > 0:
            return h * (a - b), h * (b + a)
        return h * (a + b), h * (b - a)
    return c * re - s * im, c * im + s * re


def plus(a, b):
    return b if a is None else a if b is None else a + b


def minus(a, b):
    if b is None:
        return a
    return -b if a is None else a - b


def rdft(values):
    n = len(values)
    if n == 1:
        return [(values[0], None)]
    half = n // 2
    even, odd = rdft(values[0::2]), rdft(values[1::2])
    out = []
    for k in range(half + 1):
        if k == half:
            out.append((even[0][0] - odd[0][0], None))
            break
        if k <= half // 2:
            e, o = even[k], odd[k]
        else:
            e, o = even[half - k], odd[half - k]
            e = (e[0], None if e[1] is None else -e[1])
            o = (o[0], None if o[1] is None else -o[1])
        o = times(*wpow(n, k), *o)
        out.append((plus(e[0], o[0]), plus(e[1], o[1])))
    return out


def irdft(spectrum, n):
    if n == 1:
        return [spectrum[0][0]]
    half = n // 2
    even, odd = [], []
    for k in range(half // 2 + 1):
        x = spectrum[k]
        y = spectrum[half - k]
        ym = None if y[1] is None else -y[1]
        e = (plus(x[0], y[0]), plus(x[1], ym))
        d = (minus(x[0], y[0]), minus(x[1], ym))
        c, s = wpow(n, k)
        if 2 * k == half and half > 1:
            e = (x[0] + x[0], None)
            d = (None, x[1] + x[1])
        o = d if k == 0 else times_any(c, -s, *d)
        if k == 0 or 2 * k == half:
            e, o = (e[0], None), (o[0], None)
        even.append(e)
        odd.append(o)
    if half == 1:
        even, odd = even[:1], odd[:1]
    a, b = irdft(even, half), irdft(odd, half)
    out = [None] * n
    out[0::2], out[1::2] = a, b
    return out


def times_any(c, s, re, im):
    if re is None:
        r, i = times(c, s, im, None)
        return (None if i is None else -i), r
    return times(c, s, re, im)


def part(p, odd, q):
    return p * 4 + odd * 2 + q


def kz(odd):
    return 16 + odd


def dz(odd):
    return 18 + odd


def dd(odd):
    return 24 + odd


def spread(v, pick, terms=3):
    total = None
    for k in range(terms):
        part = v.astype(BF16)
        product = jnp.dot(part, pick, preferred_element_type=F32)
        total = product if total is None else total + product
        if k < terms - 1:
            v = v - part.astype(F32)
    return total


def table(values, index):
    out = jnp.float32(values[0])
    for k in range(1, len(values)):
        out = jnp.where(index == k, jnp.float32(values[k]), out)
    return out


def kernel(
    src_hbm, init_hbm, abs_hbm, out_ref,
    src, ab, init, tbuf, sbuf, spec, kc, uu, ee, epart, ends, before, dext, va, vb, kk, join, back, f1, obuf,
    lsem, t1s, t1r, t2s, t2r, rss, rsr, wns, wnr, has, har, t3s, t3r, t4s, t4r,
):
    s = lax.axis_index("step")
    w = lax.axis_index("win")
    bx, by = s // 4, s % 4
    core = w % 2
    x0 = pl.multiple_of(bx * B, B)
    y0 = pl.multiple_of(by * B, B)
    slot = s // 2
    active = (bx + by + core) % 2 == 0

    def slot_device(f):
        return 2 * f + (f // 2 + core) % 2

    def origin(d):
        return pl.multiple_of((d // 4) * B, B), pl.multiple_of((d % 4) * B, B)

    def remote(source, target, send, recv, step=None, win=None):
        return pltpu.make_async_remote_copy(
            source, target, send, recv,
            device_id={"step": s if step is None else step, "win": w if win is None else win},
            device_id_type=MESH,
        )

    def device(shift):
        return (bx + shift[0]) % 4 * 4 + (by + shift[1]) % 4

    def counted(messages, rows, send, recv):
        size = va.at[pl.ds(0, messages), pl.ds(0, rows)]
        return remote(size, size, send, recv, step=(s + 1) % STEPS)

    load_src = pltpu.make_async_copy(src_hbm, src, lsem.at[0])
    load_abs = pltpu.make_async_copy(abs_hbm, ab, lsem.at[1])
    load_init = pltpu.make_async_copy(init_hbm.at[pl.ds(x0, B), pl.ds(y0, B)], init, lsem.at[2])
    load_src.start()
    load_abs.start()
    load_init.start()

    barrier = pltpu.get_barrier_semaphore()
    for k in range(1, STEPS):
        pl.semaphore_signal(barrier, inc=1, device_id={"step": (s + k) % STEPS, "win": w}, device_id_type=MESH)
    for k in (1, WINDOWS - 1):
        pl.semaphore_signal(barrier, inc=1, device_id={"step": s, "win": (w + k) % WINDOWS}, device_id_type=MESH)
    pl.semaphore_wait(barrier, STEPS - 1 + 2)
    load_src.wait()

    for h in range(PIECES):
        for k, shift in enumerate(OFFSETS):
            d = device(shift)
            dx, dy = origin(d)
            copy = remote(
                src.at[pl.ds(dx + h * PC, PC), pl.ds(dy, B)], tbuf.at[s, pl.ds(h * PC, PC)],
                t1s.at[0], t1r.at[h], step=d,
            )
            copy.start()
    load_init.wait()
    load_abs.wait()
    tbuf[s] = src[pl.ds(x0, B), pl.ds(y0, B), :]

    cos_of = [math.cos(2 * math.pi * f / STEPS) for f in range(SLOTS)]
    sin_of = [math.sin(2 * math.pi * f / STEPS) for f in range(SLOTS)]
    c1 = table(cos_of, slot)
    c2 = table([-1.0] + cos_of[1:], slot)
    sn = table([0.0] + sin_of[1:], slot)

    def coefficients(a, cos1, cos2, sin):
        base = a + (1.0 + 6.0 * COUPLING)
        r1 = base - GAMMA * cos1
        im = GAMMA * sin
        scale1 = COUPLING / (r1 * r1 + im * im)
        r2 = base - GAMMA * cos2
        scale2 = COUPLING / (r2 * r2 + im * im)
        return r1 * scale1, r2 * scale2, -im * scale1

    @pl.when(active)
    def _():
        def plane(x, c):
            k1, k2, kb = coefficients(ab[x], c1, c2, sn)
            for n, value in enumerate((k1, k2, kb)):
                kc[n, x, pl.ds(0, NY), :] = value
            return c

        lax.fori_loop(0, NX, plane, 0, unroll=4)
        zero = jnp.zeros((NY + 24, NZ), F32)
        zrow = jnp.zeros((8, NZ), F32)
        for p in range(2):
            for c in range(2):
                uu[p, c, 0] = zero
                uu[p, c, NX + 1] = zero

        def rows(x, c):
            for p in range(2):
                for q in range(2):
                    uu[p, q, x, pl.ds(0, 8), :] = zrow
                    uu[p, q, x, pl.ds(40, 8), :] = zrow
            return c

        lax.fori_loop(1, NX + 1, rows, 0, unroll=4)

    first_window = jnp.where(w == 0, jnp.float32(1.0), jnp.float32(0.0))

    def transform(x, c):
        values = []
        for t in range(STEPS):
            v = tbuf[t, x]
            if t == 0:
                v = v + first_window * init[x]
            values.append(v * (GAMMA**t / COUPLING))
        out = rdft(values)
        sbuf[0, 0, x], sbuf[0, 1, x] = out[0][0], out[8][0]
        for f in range(1, SLOTS):
            sbuf[f, 0, x], sbuf[f, 1, x] = out[f]
        return c

    def to_slot(k, h, shift):
        d = device(shift)
        half = pl.ds(x0 + h * PC, PC)
        return remote(
            sbuf.at[d // 2, :, pl.ds(h * PC, PC)], spec.at[:, half, pl.ds(y0, B)],
            t2s.at[0], t2r.at[h], step=d,
        )

    def send_to_slots(h):
        @pl.when(active)
        def _():
            for k, shift in enumerate(EVEN):
                to_slot(k, h, shift).start()

        @pl.when(jnp.logical_not(active))
        def _():
            for k, shift in enumerate(ODD):
                to_slot(k, h, shift).start()

    for h in range(PIECES):
        counted(STEPS - 1, PC * B, t1s.at[0], t1r.at[h]).wait_recv()
        lax.fori_loop(h * PC, (h + 1) * PC, transform, 0)
        send_to_slots(h)

    wide_lane = lax.broadcasted_iota(jnp.int32, (3 * B, NZ), 1)
    low = wide_lane < HALF
    pick_z = lax.broadcasted_iota(jnp.int32, (NZ, 2 * NZ), 0)
    pick_l = lax.broadcasted_iota(jnp.int32, (NZ, 2 * NZ), 1)
    pick = jnp.where(pick_z == 2 * (pick_l % HALF) + pick_l // NZ, 1.0, 0.0).astype(BF16)
    join_r = lax.broadcasted_iota(jnp.int32, (2 * NZ, 2 * NZ), 0)
    join_c = lax.broadcasted_iota(jnp.int32, (2 * NZ, 2 * NZ), 1)
    goes = ((join_r // HALF) % 2) * NZ + 2 * (join_r % HALF) + join_r // NZ
    join[...] = jnp.where(join_c == goes, 1.0, 0.0).astype(BF16)

    def at(a, b):
        return jnp.where(low, jnp.float32(a), jnp.float32(b))

    def turned(v, odd):
        lanes = wide_lane[: v.shape[0]] % HALF
        if odd:
            return jnp.where(lanes == 0, 0.0, pltpu.roll(v, 1, 1))
        return jnp.where(lanes == HALF - 1, 0.0, pltpu.roll(v, NZ - 1, 1))

    def wide_plane(i, c):
        gx = x0 - B + i
        inx = jnp.logical_and(gx >= 0, gx < NX)
        gxc = jnp.clip(gx, 0, NX - 1)
        tiles, keeps = [], []
        for b in range(3):
            gy = by - 1 + b
            inside = jnp.logical_and(inx, jnp.logical_and(gy >= 0, gy < 4))
            keep = jnp.where(inside, jnp.float32(COUPLING), jnp.float32(0.0))
            tiles.append(ab[gxc, pl.ds(pl.multiple_of(jnp.clip(gy, 0, 3) * B, B), B), :])
            keeps.append(jnp.full((B, NZ), keep, F32))
        both = spread(jnp.concatenate(tiles, 0), pick)
        keep = jnp.concatenate(keeps, 0)
        rows = pl.ds(pl.multiple_of(i * PITCH, PITCH), 3 * B)
        for odd in range(2):
            base = both[:, odd * NZ : (odd + 1) * NZ] + (1.0 + 6.0 * COUPLING)
            for p in range(PAIRS):
                q = p + PAIRS
                r = base - at(GAMMA * cos_of[p], GAMMA * cos_of[q])
                im = at(GAMMA * sin_of[p], GAMMA * sin_of[q])
                scale = keep / (r * r + im * im)
                ka, kb = r * scale, -im * scale
                if p == 0:
                    r2 = base - at(-GAMMA, GAMMA * cos_of[q])
                    k2 = r2 * (keep / (r2 * r2 + im * im))
                    kk[kz(odd), rows, :] = k2
                kk[part(p, odd, 0), rows, :], kk[part(p, odd, 1), rows, :] = ka, kb
                if p == 2:
                    kk[4 + kz(odd), rows, :], kk[4 + dz(odd), rows, :] = ka, jnp.zeros_like(ka)
        return c

    lax.fori_loop(1, 3 * B - 1, wide_plane, 0)

    @pl.when(active)
    def _():
        for c in range(2):
            spec[c, pl.ds(x0, B), pl.ds(y0, B), :] = sbuf[slot, c]
        for h in range(PIECES):
            counted(STEPS - 1, 2 * PC * B, t2s.at[0], t2r.at[h]).wait_recv()

            def begin(i, c, h=h):
                for m in range(PC):
                    x = i * B + h * PC + m
                    k1, k2, kb = (kc[n, x, pl.ds(0, NY), :] for n in range(3))
                    s0, s1 = (spec[n, x, pl.ds(0, NY), :] for n in range(2))
                    uu[0, 0, x + 1, pl.ds(8, NY), :] = k1 * s0 - kb * s1
                    uu[0, 1, x + 1, pl.ds(8, NY), :] = k2 * s1 + kb * s0
                return c

            lax.fori_loop(0, NX // B, begin, 0)

    lane = lax.broadcasted_iota(jnp.int32, (8, NZ), 1)

    def z_sum(v):
        n = v.shape[0]
        at = jnp.concatenate([lane] * (n // 8), 0) if n > 8 else lane
        below = jnp.where(at == 0, 0.0, pltpu.roll(v, 1, 1))
        above = jnp.where(at == NZ - 1, 0.0, pltpu.roll(v, NZ - 1, 1))
        return below + above

    p_end = 2.0 / (16 * GAMMA**15)
    ends_re = table([0.5 * p_end] + [p_end * v for v in cos_of[1:]], slot)
    ends_im = table([-0.5 * p_end] + [p_end * v for v in sin_of[1:]], slot)

    @pl.when(active)
    def _():
        def sweep(k, c):
            old = k % 2

            def load(q, px, py):
                return uu[old, q, px, pl.ds(py, NY), :]

            for x in range(NX):
                nb = []
                for q in range(2):
                    t = load(q, x, 8) + load(q, x + 2, 8)
                    t = t + (load(q, x + 1, 7) + load(q, x + 1, 9))
                    nb.append(t + z_sum(load(q, x + 1, 8)))
                k1, k2, kb = (kc[n, x, pl.ds(0, NY), :] for n in range(3))
                s0, s1 = (spec[n, x, pl.ds(0, NY), :] + nb[n] for n in range(2))
                uu[1 - old, 0, x + 1, pl.ds(8, NY), :] = k1 * s0 - kb * s1
                uu[1 - old, 1, x + 1, pl.ds(8, NY), :] = k2 * s1 + kb * s0
            return c

        lax.fori_loop(0, SWEEPS - 1, sweep, 0)

        def end(x, c):
            rows = pl.ds(8, NY)
            ee[x] = ends_re * uu[1, 0, x + 1, rows, :] + ends_im * uu[1, 1, x + 1, rows, :]
            return c

        lax.fori_loop(0, NX, end, 0, unroll=4)

        for k, shift in enumerate(OFFSETS):
            d = device(shift)
            dx, dy = origin(d)
            remote(ee.at[pl.ds(dx, B), pl.ds(dy, B)], epart.at[slot], rss.at[0], rsr.at[0], step=d).start()
        epart[slot] = ee[pl.ds(x0, B), pl.ds(y0, B), :]

    def from_slot(k, h, shift):
        d = device(shift)
        dx, dy = origin(d)
        return remote(
            uu.at[1, :, pl.ds(dx + h * PB + 1, PB), pl.ds(pl.multiple_of(dy + 8, 8), B)],
            f1.at[slot, :, pl.ds(h * PB, PB)], t3s.at[0], t3r.at[h], step=d,
        )

    def return_field(h):
        @pl.when(active)
        def _():
            for k, shift in enumerate(OFFSETS):
                from_slot(k, h, shift).start()
            for c in range(2):
                f1[slot, c, pl.ds(h * PB, PB)] = uu[
                    1, c, pl.ds(x0 + h * PB + 1, PB), pl.ds(pl.multiple_of(y0 + 8, 8), B), :
                ]

    return_field(0)

    def slots_wait(rows, send, recv):
        pl.when(active)(lambda: counted(SLOTS - 1, rows, send, recv).wait_recv())
        pl.when(jnp.logical_not(active))(lambda: counted(SLOTS, rows, send, recv).wait_recv())

    slots_wait(B * B, rss.at[0], rsr.at[0])
    for x in range(B):
        total = epart[0, x]
        for f in range(1, SLOTS):
            total = total + epart[f, x]
        ends[x] = total

    to_next = remote(ends, before, wns.at[0], wnr.at[0], win=(w + 1) % WINDOWS)
    to_next.start()
    to_next.wait_recv()
    later_window = jnp.where(w == 0, jnp.float32(0.0), jnp.float32(1.0 / COUPLING))
    change = later_window * before[...] - (ALPHA / COUPLING) * ends[...]
    pack = jnp.where(
        pick_z[:, :NZ] == 2 * (pick_l[:, :NZ] % HALF) + pick_l[:, :NZ] // HALF, 1.0, 0.0
    ).astype(BF16)
    dext[pl.ds(B, B), pl.ds(B, B), :] = spread(change.reshape(B * B, NZ), pack, 2).reshape(B, B, NZ)

    shifts = [(0, 1), (0, -1), (1, 0), (-1, 0), (1, 1), (-1, -1), (1, -1), (-1, 1)]
    for k, (i, j) in enumerate(shifts):
        d = ((bx + i + 4) % 4) * 4 + (by + j + 4) % 4
        n = B - abs(i) * (1 + abs(j))
        first = B if i < 1 else 2 * B - n
        remote(
            dext.at[pl.ds(first, n), pl.ds(B, B)],
            dext.at[pl.ds(first - B * i, n), pl.ds(B - B * j, B)],
            has.at[0], har.at[k // 4], step=d,
        ).start()

    def wide_start(i, j):
        row = B - B * j
        mask = low[:B]
        n = B - abs(i) * (1 + abs(j))
        first = (B if i < 1 else 2 * B - n) - B * i
        for plane in range(first, first + n):
            rows = pl.ds(plane * PITCH + row, B)
            v = dext[plane, pl.ds(row, B), :]
            swapped = pltpu.roll(v, HALF, 1)
            d = [jnp.where(mask, v, swapped), jnp.where(mask, swapped, v)]
            for odd in range(2):
                kk[dd(odd), rows, :] = d[odd]
                kk[dz(odd), rows, :] = jnp.where(mask, d[odd], 0.0)
                for p in range(PAIRS):
                    second = kk[part(p, odd, 1), rows, :]
                    if p == 0:
                        second = jnp.where(mask, kk[kz(odd), rows, :], second)
                    va[part(p, odd, 0), rows, :] = kk[part(p, odd, 0), rows, :] * d[odd]
                    va[part(p, odd, 1), rows, :] = second * d[odd]

    wide_start(0, 0)
    for k in range(2):
        counted(4, (60, 48)[k], has.at[0], har.at[k]).wait_recv()
        for i, j in shifts[4 * k : 4 * k + 4]:
            wide_start(i, j)

    return_field(1)

    zero_row = s // STEPS
    for k in range(SWEEPS - 1):
        reach = SWEEPS - 2 - k
        vo, vn = (va, vb) if k % 2 == 0 else (vb, va)
        places = []
        for i in range(B - reach, 2 * B + reach):
            rest = reach - max(B - i, i - 2 * B + 1, 0)
            places += [i * PITCH + B - rest + 8 * tile for tile in range(-(-(B + 2 * rest) // 8))]

        def wide(g, c, vo=vo, vn=vn, places=places):
            for place in places:
                start = place + zero_row
                rows = pl.ds(start, 8)
                around = [pl.ds(start + shift, 8) for shift in (-PITCH, PITCH, -1, 1)]
                for p in range(2):
                    first = 8 * g
                    middle = [[vo[first + part(p, odd, q), rows, :] for q in range(2)] for odd in range(2)]
                    for odd in range(2):
                        nb = []
                        for q in range(2):
                            here, other = first + part(p, odd, q), middle[1 - odd][q]
                            t = vo[here, around[0], :] + vo[here, around[1], :]
                            t = t + (vo[here, around[2], :] + vo[here, around[3], :])
                            nb.append((t + other) + turned(other, 1 - odd))
                        ka, kb = kk[first + part(p, odd, 0), rows, :], kk[first + part(p, odd, 1), rows, :]
                        s0, s1, k2 = kk[dd(odd), rows, :] + nb[0], nb[1], ka
                        if p == 0:
                            s1, k2 = s1 + kk[4 * g + dz(odd), rows, :], kk[4 * g + kz(odd), rows, :]
                        vn[first + part(p, odd, 0), rows, :] = ka * s0 - kb * s1
                        vn[first + part(p, odd, 1), rows, :] = k2 * s1 + kb * s0
            return c

        lax.fori_loop(0, 2, wide, 0)

    def natural(h):
        mixed = []
        for p in range(PAIRS):
            for q in range(2):
                sides = [
                    jnp.concatenate(
                        [vb[part(p, odd, q), pl.ds((B + h * PT + x) * PITCH + B, B), :] for x in range(PT)], 0
                    )
                    for odd in range(2)
                ]
                mixed.append(jnp.concatenate(sides, 1))
        mixed = jnp.concatenate(mixed, 0)
        high = mixed.astype(BF16)
        rest = (mixed - high.astype(F32)).astype(BF16)
        n = mixed.shape[0]
        both = jnp.dot(jnp.concatenate([high, rest], 0), join[...], preferred_element_type=F32)
        back[...] = both[:n] + both[n:]

    def untransform(h):
        for x in range(PT):
            total = []
            for f in range(SLOTS):
                lanes = pl.ds(f // PAIRS * NZ, NZ)
                total.append(
                    [
                        f1[f, q, h * PT + x]
                        + back[pl.ds(((f % PAIRS * 2 + q) * PT + x) * B, B), lanes]
                        for q in range(2)
                    ]
                )
            spectrum = [(total[0][0], None)] + [tuple(v) for v in total[1:]] + [(total[0][1], None)]
            values = irdft(spectrum, STEPS)
            for t in range(STEPS):
                obuf[t, h * PT + x] = values[t]

    def to_step(k, h, shift):
        d = device(shift)
        return remote(
            obuf.at[d, pl.ds(h * PT, PT)], out_ref.at[pl.ds(x0 + h * PT, PT), pl.ds(y0, B)],
            t4s.at[0], t4r.at[0], step=d,
        )

    for h in range(TURNS):
        natural(h)
        if h % (TURNS // PARTS) == 0:
            slots_wait(2 * PB * B, t3s.at[0], t3r.at[h // (TURNS // PARTS)])
        untransform(h)
        for k, shift in enumerate(OFFSETS):
            to_step(k, h, shift).start()
        out_ref[pl.ds(x0 + h * PT, PT), pl.ds(y0, B), :] = obuf[s, pl.ds(h * PT, PT)]

    counted(STEPS - 1, B * B, t1s.at[0], t1r.at[0]).wait_send()
    to_next.wait_send()
    counted(8, 54, has.at[0], har.at[0]).wait_send()

    @pl.when(active)
    def _():
        counted(SLOTS - 1, 2 * B * B, t2s.at[0], t2r.at[0]).wait_send()
        counted(STEPS - 1, B * B, rss.at[0], rsr.at[0]).wait_send()
        counted(STEPS - 1, 2 * B * B, t3s.at[0], t3r.at[0]).wait_send()

    @pl.when(jnp.logical_not(active))
    def _():
        counted(SLOTS, 2 * B * B, t2s.at[0], t2r.at[0]).wait_send()

    last = counted(STEPS - 1, B * B, t4s.at[0], t4r.at[0])
    last.wait_send()
    last.wait_recv()


def per_device(initial_state, source, absorption):
    grid = (NX, NY, NZ)
    vmem = lambda *shape: pltpu.VMEM(shape, F32)
    dma = lambda *n: pltpu.SemaphoreType.DMA(n)
    result = pl.pallas_call(
        kernel,
        out_shape=pltpu.VMEM(grid, F32),
        in_specs=[pl.BlockSpec(memory_space=pl.ANY)] * 3,
        out_specs=pl.BlockSpec(memory_space=pltpu.VMEM),
        scratch_shapes=[
            vmem(*grid),
            vmem(*grid),
            vmem(B, B, NZ),
            vmem(STEPS, B, B, NZ),
            vmem(SLOTS, 2, B, B, NZ),
            vmem(2, NX, NY + 8, NZ),
            vmem(4, NX, NY + 8, NZ),
            vmem(2, 2, NX + 4, NY + 24, NZ),
            vmem(*grid),
            vmem(SLOTS, B, B, NZ),
            vmem(B, B, NZ),
            vmem(B, B, NZ),
            vmem(3 * B, 4 * B, NZ),
            vmem(16, 3 * B * PITCH + 8, NZ),
            vmem(16, 3 * B * PITCH + 8, NZ),
            vmem(28, 3 * B * PITCH + 8, NZ),
            pltpu.VMEM((2 * NZ, 2 * NZ), BF16),
            vmem(2 * PAIRS * PT * B, 2 * NZ),
            vmem(SLOTS, 2, B, B, NZ),
            vmem(STEPS, B, B, NZ),
            dma(3),
            dma(1), dma(PIECES),
            dma(1), dma(PIECES),
            dma(1), dma(1),
            dma(1), dma(1),
            dma(1), dma(2),
            dma(1), dma(PARTS),
            dma(1), dma(1),
        ],
        compiler_params=pltpu.CompilerParams(
            collective_id=0, has_side_effects=True, vmem_limit_bytes=60 * 2**20,
        ),
        name="windows",
    )(source[0, 0], initial_state, absorption)
    moment = lax.axis_index("step").astype(F32)
    return (result * (GAMMA ** (-moment) / STEPS))[None, None]


def solution(mesh):
    return jax.shard_map(
        per_device,
        mesh=mesh,
        in_specs=(P(), P("win", "step", None, None, None), P()),
        out_specs=P("win", "step", None, None, None),
        check_vma=False,
    )
```
